32 devices in a mesh: shard: 8 (over z, y), width: 4 (over x, core).
Axes of the slice: x: 2, y: 2, z: 4, core: 2. Of those that a mesh axis runs over, the one named last changes fastest.
Arguments:
- one_query: float32 [3584, 4096], P('shard', 'width'), may hold values from -0.125 to 0.125
- other_query: float32 [3584, 4096], P('shard', 'width'), may hold values from -0.09375 to 0.09375
- one_key: float32 [3584, 2048], P('shard', 'width'), may hold values from -0.125 to 0.125
- other_key: float32 [3584, 2048], P('shard', 'width'), may hold values from -0.09375 to 0.09375
- one_value: float32 [3584, 2048], P('shard', 'width'), may hold values from -0.125 to 0.125
- other_value: float32 [3584, 2048], P('shard', 'width'), may hold values from -0.09375 to 0.09375
- mix_share: float32 [3584], P('shard'), may hold values from 0.2 to 0.8
- norm_gain: float32 [3584], P('shard'), may hold values from 0.25 to 1.75
Outputs:
- final_query: bfloat16 [3584, 4096], P(None, 'width')
- final_key: bfloat16 [3584, 2048], P(None, 'width')
- final_value: bfloat16 [3584, 2048], P(None, 'width')
- scale_query: float32 [4096], P('width')
- scale_key: float32 [2048], P('width')
- scale_value: float32 [2048], P('width')
The draws below stay inside these ranges and needn't reach their ends.
All inputs are finite; a program needn't handle non-finite values.
Results may differ from the reference program's by a relative error of at most 0.001.
Values may be sent and summed in bfloat16 or wider, within the bound.
A program may use at most 128 MiB of HBM per device.

```python
import jax
import jax.numpy as jnp
from jax import lax

D_MODEL = 3584
Q_DIM = 4096
KV_DIM = 2048


def raised(array, own_key, source, target, blocks, factor):
    def block_of(axis_at):
        return (jnp.arange(array.shape[axis_at]) // (array.shape[axis_at] // blocks)).reshape((-1,) + (1,) * (array.ndim - 1 - axis_at))

    first = jax.random.permutation(own_key, blocks)[block_of(target)]
    second = (block_of(target) + blocks // 2) % blocks
    return jnp.where((block_of(source) == first) | (block_of(source) == second), factor * array, array)


def shard_levels(own_key, dims, cuts, low, top_value):
    loudness, own = 1.0, jax.random.fold_in(own_key, 6)
    for position, parts in cuts:
        draws = jnp.exp(jax.random.uniform(jax.random.fold_in(own, position), (parts,), jnp.float32, low / len(cuts), top_value / len(cuts)))
        loudness = loudness * jnp.repeat(draws, dims[position] // parts).reshape([-1 if axis == position else 1 for axis in range(len(dims))])
    return loudness


def normal_values(rng, shape, width, most, pieces=(), dtype=jnp.bfloat16):
    factor_of = shard_levels(rng, shape, pieces, -0.22, 0.18) if pieces else 1.0
    result = jax.random.normal(rng, shape, jnp.float32) * width * factor_of
    return jnp.minimum(jnp.maximum(result, -most), most).astype(dtype)


def bell_draw_with(own_key, extent, scale, most, cuts, heavy, kind=jnp.bfloat16):
    values = scale * jax.random.normal(own_key, extent, jnp.float32)
    if cuts:
        values = values * shard_levels(own_key, extent, cuts, -0.22, 0.18)
    return jnp.clip(raised(values, jax.random.fold_in(own_key, 3), *heavy), -most, most).astype(kind)


def setup_inputs(seed: int = 0) -> dict:
    key_list = jax.random.split(jax.random.key(seed), 9)
    one_query = bell_draw_with(key_list[0], (D_MODEL, Q_DIM), D_MODEL ** -0.5, 0.125, ((0, 8), (1, 4)), (0, 1, 8, 2.0), jnp.float32)
    other_query = normal_values(key_list[1], (D_MODEL, Q_DIM), D_MODEL ** -0.5, 0.09375, ((0, 8), (1, 4)), jnp.float32)
    one_key = bell_draw_with(key_list[2], (D_MODEL, KV_DIM), D_MODEL ** -0.5, 0.125, ((0, 8), (1, 4)), (0, 1, 8, 2.0), jnp.float32)
    other_key = normal_values(key_list[3], (D_MODEL, KV_DIM), D_MODEL ** -0.5, 0.09375, ((0, 8), (1, 4)), jnp.float32)
    one_value = bell_draw_with(key_list[4], (D_MODEL, KV_DIM), D_MODEL ** -0.5, 0.125, ((0, 8), (1, 4)), (0, 1, 8, 2.0), jnp.float32)
    other_value = normal_values(key_list[5], (D_MODEL, KV_DIM), D_MODEL ** -0.5, 0.09375, ((0, 8), (1, 4)), jnp.float32)
    mix_share = jnp.clip(0.2 + 0.6 * jax.random.uniform(key_list[6], (D_MODEL,), jnp.float32) ** shard_levels(key_list[6], (D_MODEL,), ((0, 8),), -0.2, 0.2), 0.2, 0.8)
    norm_gain = jnp.clip(1.0 + 0.15 * jax.random.normal(key_list[7], (D_MODEL,), jnp.float32), 0.25, 1.75)
    return {"one_query": one_query, "other_query": other_query, "one_key": one_key, "other_key": other_key, "one_value": one_value, "other_value": other_value, "mix_share": mix_share, "norm_gain": norm_gain}


def reference(one_query, other_query, one_key, other_key, one_value, other_value, mix_share, norm_gain):
    result_query = mix_share[:, None] * one_query + (1.0 - mix_share[:, None]) * other_query
    result_key = mix_share[:, None] * one_key + (1.0 - mix_share[:, None]) * other_key
    result_value = mix_share[:, None] * one_value + (1.0 - mix_share[:, None]) * other_value
    result_gained_query = result_query * norm_gain[:, None]
    result_gained_key = result_key * norm_gain[:, None]
    result_gained_value = result_value * norm_gain[:, None]
    scale_query = jnp.sqrt(lax.optimization_barrier(jnp.sum(result_gained_query * result_gained_query, axis=0)))
    final_query = (result_gained_query / scale_query).astype(jnp.bfloat16)
    scale_key = jnp.sqrt(lax.optimization_barrier(jnp.sum(result_gained_key * result_gained_key, axis=0)))
    final_key = (result_gained_key / scale_key).astype(jnp.bfloat16)
    scale_value = jnp.sqrt(lax.optimization_barrier(jnp.sum(result_gained_value * result_gained_value, axis=0)))
    final_value = (result_gained_value / scale_value).astype(jnp.bfloat16)
    return (final_query, final_key, final_value, scale_query, scale_key, scale_value)
```

```python
import functools
import heapq

import jax
import jax.numpy as jnp
from jax import lax
from jax.experimental import pallas as pl
from jax.experimental.pallas import tpu as pltpu
from jax.sharding import PartitionSpec as P

MESH = pl.DeviceIdType.MESH
ROWS = 16
TILE = 8
LANES = 128
EARLY = (8, 24)
UP, DOWN, ACROSS = range(3)
PARTS = 3


def plain(one_query, other_query, one_key, other_key, one_value, other_value, mix_share, norm_gain):
    result_query = mix_share[:, None] * one_query + (1.0 - mix_share[:, None]) * other_query
    result_key = mix_share[:, None] * one_key + (1.0 - mix_share[:, None]) * other_key
    result_value = mix_share[:, None] * one_value + (1.0 - mix_share[:, None]) * other_value
    result_gained_query = result_query * norm_gain[:, None]
    result_gained_key = result_key * norm_gain[:, None]
    result_gained_value = result_value * norm_gain[:, None]
    total_query, total_key, total_value = lax.psum(
        (
            jnp.sum(result_gained_query * result_gained_query, axis=0),
            jnp.sum(result_gained_key * result_gained_key, axis=0),
            jnp.sum(result_gained_value * result_gained_value, axis=0),
        ),
        "shard",
    )
    scale_query = jnp.sqrt(total_query)
    scale_key = jnp.sqrt(total_key)
    scale_value = jnp.sqrt(total_value)
    narrow_query, narrow_key, narrow_value = (
        (result_gained_query / scale_query).astype(jnp.bfloat16),
        (result_gained_key / scale_key).astype(jnp.bfloat16),
        (result_gained_value / scale_value).astype(jnp.bfloat16),
    )
    final_query, final_key, final_value = (
        lax.all_gather(narrow_query, "shard", axis=0, tiled=True),
        lax.all_gather(narrow_key, "shard", axis=0, tiled=True),
        lax.all_gather(narrow_value, "shard", axis=0, tiled=True),
    )
    return (final_query, final_key, final_value, scale_query, scale_key, scale_value)


def cuts(start, end, parts, unit):
    edges = [start + (end - start) // unit * part // parts * unit for part in range(parts)] + [end]
    return [(low, high - low) for low, high in zip(edges, edges[1:])]


def plan(rows):
    early = sum(EARLY)
    half = rows // 2 // ROWS * ROWS
    near = [(0, early)] + cuts(early, half, 2, ROWS)
    return near + [(half, rows - half)], len(near)


def sending(level, line, pieces, order):
    own = sum(size for _, size in pieces[1:])
    sent = [own if ok else 0 for ok in (level < line - 1, level > 0, True)]
    for _, _, c, ways, _ in order[level]:
        for way in ways:
            sent[way] += pieces[c][1]
    return sent


def folded(amount, rows, n):
    return next((d for d in range(1, n + 1) if amount % (d * TILE) == 0 and amount // d <= rows), None)


def fits(n, rows):
    if n % 2 or n < 4 or rows % ROWS or rows < 4 * sum(EARLY):
        return False
    pieces, near = plan(rows)
    order = relays(n // 2, pieces, near)
    return all(not amount or folded(amount, rows, n) for z in range(n // 2) for amount in sending(z, n // 2, pieces, order))


def stages(rows, lead):
    return [(0, lead)] + cuts(lead, rows, PARTS, ROWS)


def relays(line, pieces, near):
    latency = 3 * TILE
    events, free, order = [], {}, [[] for _ in range(line)]

    def send(time, z, way, column, source, c):
        start = max(time, free.get((z, way), 0))
        free[z, way] = start + pieces[c][1]
        target = (z + 1, z - 1, z)[way]
        heapq.heappush(events, (free[z, way] + latency, len(events), target, column ^ (way == ACROSS), source, c))

    def onward(z, column, source, c):
        along = [UP] if (source < z or source == z == 0) and z < line - 1 else []
        along += [DOWN] if (source > z or source == z == line - 1) and z > 0 else []
        crosses = source not in (0, line - 1) or c < near
        if column == 0:
            return along + ([ACROSS] if crosses else [])
        return [] if crosses else along

    for z in range(line):
        for c in range(1, len(pieces)):
            for way, ok in ((UP, z < line - 1), (DOWN, z > 0), (ACROSS, True)):
                if ok:
                    send(0, z, way, 0, z, c)
        for way, ok in ((UP, z < line - 1), (DOWN, z > 0), (ACROSS, True)):
            if ok:
                target = (z + 1, z - 1, z)[way]
                heapq.heappush(events, (0, len(events), target, int(way == ACROSS), z, 0))
    serial = 0
    while events:
        time, _, z, column, source, c = heapq.heappop(events)
        ways = onward(z, column, source, c)
        direct = c == 0 and (abs(source - z) == 1 and column == 0 or source == z)
        order[z].append((column, source, c, ways, direct))
        for way in ways:
            start = max(time, free.get((z, way), 0))
            free[z, way] = start + pieces[c][1]
            serial += 1
            heapq.heappush(events, (free[z, way] + latency, 10**6 + serial, (z + 1, z - 1, z)[way], column ^ (way == ACROSS), source, c))
    return order


def gather_kernel(n, widths, *refs):
    (share_hbm, gain_hbm), ins, (buf, scale_ref, share_ref, gain_ref, first, second, left, right, sums, early, row_sem, in_sem, sum_sem, early_send, early_recv, send_sem, recv_sem) = refs[:2], refs[2:8], refs[8:]
    rows = first.shape[0]
    total = sum(widths)
    line = n // 2
    me = lax.axis_index("shard")
    z, y = me // 2, me % 2
    other = z * 2 + 1 - y
    pieces, near = plan(rows)
    order = relays(line, pieces, near)
    lead = sum(EARLY)
    starts = [sum(widths[:i]) for i in range(len(widths))]

    vectors = [
        pltpu.make_async_copy(source, dest, row_sem.at[i])
        for i, (source, dest) in enumerate(((share_hbm, share_ref), (gain_hbm, gain_ref)))
    ]
    for copy in vectors:
        copy.start()
    loads = []
    parts = stages(rows, lead)
    for p, (low, size) in enumerate(parts):
        for i, ref in enumerate(ins):
            dest = (first, second)[i % 2].at[pl.ds(low, size), pl.ds(starts[i // 2], widths[i // 2])]
            pltpu.make_async_copy(ref.at[pl.ds(low, size), :], dest, in_sem.at[p, i % 2]).start()
        whole = [ref.at[pl.ds(low, size), :] for ref in (first, second)]
        loads.append([pltpu.make_async_copy(ref, ref, in_sem.at[p, i]) for i, ref in enumerate(whole)])

    barrier = pltpu.get_barrier_semaphore()
    for step in range(1, n):
        pl.semaphore_signal(barrier, inc=1, device_id={"shard": lax.rem(me + step, n)}, device_id_type=MESH)

    for copy in vectors:
        copy.wait()
    for low in range(0, rows, LANES):
        size = min(LANES, rows - low)
        share, gain = share_ref[:, low:low + size], gain_ref[:, low:low + size]
        for ref, row in ((left, share * gain), (right, (1.0 - share) * gain)):
            ref[pl.ds(low, size), :] = jnp.transpose(jnp.broadcast_to(row, (LANES, size)))

    def mixed(block, acc):
        at = pl.ds(pl.multiple_of(block * ROWS, ROWS), ROWS)
        ours, theirs = (jnp.concatenate([ref[at, :]] * 4, axis=1) for ref in (left, right))
        out = []
        for i in range(len(acc)):
            cols = pl.ds(i * 512, 512)
            value = ours * first[at, cols] + theirs * second[at, cols]
            first[at, cols] = value
            square = value * value
            out.append(acc[i] + square[:8] + square[8:])
        return tuple(out)

    up, down, always = z < line - 1, z > 0, z >= 0
    conditions = (up, down, always)
    targets = (jnp.minimum(z + 1, line - 1) * 2 + y, jnp.maximum(z - 1, 0) * 2 + y, other)

    def early_copy(way, low, size):
        return pltpu.make_async_remote_copy(
            src_ref=first.at[pl.ds(low, size), :], dst_ref=early.at[way, pl.ds(low, size), :],
            send_sem=early_send.at[way], recv_sem=early_recv.at[way],
            device_id={"shard": targets[way]}, device_id_type=MESH)

    def start_early(k):
        for way, condition in enumerate(conditions):
            @pl.when(condition)
            def _():
                early_copy(way, sum(EARLY[:k]), EARLY[k]).start()

    acc = tuple(jnp.zeros((8, 512), jnp.float32) for _ in range(total // 512))
    for p, (group, (low, size)) in enumerate(zip(loads, parts)):
        for copy in group:
            copy.wait()
        acc = lax.fori_loop(low // ROWS, (low + size) // ROWS, mixed, acc)
        if p == 1:
            pl.semaphore_wait(barrier, n - 1)
            start_early(0)
    for i, value in enumerate(acc):
        sums[me, :, pl.ds(i * 512, 512)] = jnp.sum(value, axis=0, keepdims=True)

    def sum_copy(target, ref):
        return pltpu.make_async_remote_copy(
            src_ref=ref, dst_ref=ref, send_sem=sum_sem.at[0], recv_sem=sum_sem.at[1],
            device_id={"shard": target}, device_id_type=MESH)

    peers = [jnp.where(z < line // 2, line - 1 - k, k) * 2 + side for k in range(line) for side in (1 - y, y)]
    for peer in peers:
        @pl.when(peer != me)
        def _():
            sum_copy(peer, sums.at[me]).start()
    for k in range(1, len(EARLY)):
        start_early(k)

    everyone = sum_copy(other, sums.at[pl.ds(0, n - 1)])
    everyone.wait_recv()
    whole = sums[0]
    for source in range(1, n):
        whole = whole + sums[source]
    scale = jnp.sqrt(whole)
    scale_ref[...] = scale
    inverse = jnp.broadcast_to(1.0 / scale, (8, total))

    def scaled(source, ref):
        def step(block, carry):
            at = pl.ds(pl.multiple_of(block * ROWS, ROWS), ROWS)
            for i in range(total // 512):
                cols = pl.ds(i * 512, 512)
                wide = jnp.concatenate([inverse[:, i * 512:(i + 1) * 512]] * 2, axis=0)
                buf[source, at, cols] = (ref[at, cols] * wide).astype(buf.dtype)
            return carry
        return step

    def copy(way, source, c):
        low, size = pieces[c]
        ref = buf.at[source, pl.ds(low, size), :]
        return pltpu.make_async_remote_copy(
            src_ref=ref, dst_ref=ref, send_sem=send_sem.at[way], recv_sem=recv_sem.at[source, c],
            device_id={"shard": targets[way]}, device_id_type=MESH)

    def issue_own(c):
        for way, condition in enumerate(conditions):
            @pl.when(condition)
            def _():
                copy(way, me, c).start()

    for c, (low, size) in enumerate(pieces[1:], 1):
        lax.fori_loop(low // ROWS, (low + size) // ROWS, scaled(me, first), 0)
        if c == 1:
            lax.fori_loop(0, lead // ROWS, scaled(me, first), 0)
            issue_own(c)
        if c > 2:
            issue_own(c - 1)
    issue_own(len(pieces) - 1)

    for way, (condition, source) in enumerate(((down, me - 2), (up, me + 2), (always, other))):
        @pl.when(condition)
        def _():
            early_copy(way, 0, lead).wait_recv()
            lax.fori_loop(0, lead // ROWS, scaled(source, early.at[way]), 0)

    for level in range(line):
        @pl.when(z == level)
        def _():
            for column, at, c, ways, direct in order[level]:
                source = at * 2 + (1 - y if column else y)
                if not direct:
                    copy(ACROSS, source, c).wait_recv()
                for way in ways:
                    copy(way, source, c).start()
            for way, amount in enumerate(sending(level, line, pieces, order)):
                if amount:
                    depth = folded(amount, rows, n)
                    ref = buf.at[pl.ds(0, depth), pl.ds(0, amount // depth), :]
                    pltpu.make_async_remote_copy(
                        src_ref=ref, dst_ref=ref, send_sem=send_sem.at[way], recv_sem=recv_sem.at[0, 0],
                        device_id={"shard": targets[way]}, device_id_type=MESH).wait_send()

    for way, condition in enumerate(conditions):
        @pl.when(condition)
        def _():
            early_copy(way, 0, lead).wait_send()
    everyone.wait_send()


def store_kernel(widths, buf, scale_ref, *refs):
    outs, scales, sem = refs[:3], refs[3:6], refs[6]
    copies = []
    start = 0
    for i, width in enumerate(widths):
        copies.append(pltpu.make_async_copy(buf.at[:, :, pl.ds(start, width)], outs[i], sem.at[0, i]))
        copies.append(pltpu.make_async_copy(scale_ref.at[:, pl.ds(start, width)], scales[i], sem.at[1, i]))
        start += width
    for copy in copies:
        copy.start()
    for copy in copies:
        copy.wait()


def routed(n, one_query, other_query, one_key, other_key, one_value, other_value, mix_share, norm_gain):
    widths = (one_query.shape[1], one_key.shape[1], one_value.shape[1])
    rows, total = one_query.shape[0], sum(widths)
    pieces = len(plan(rows)[0])
    lead = sum(EARLY)
    vmem = pl.BlockSpec(memory_space=pltpu.VMEM)
    hbm = pl.BlockSpec(memory_space=pl.ANY)
    buf, scale = pl.pallas_call(
        functools.partial(gather_kernel, n, widths),
        out_shape=(pltpu.VMEM((n, rows, total), jnp.bfloat16), pltpu.VMEM((1, total), jnp.float32)),
        in_specs=[hbm] * 8,
        out_specs=(vmem, vmem),
        scratch_shapes=[
            pltpu.VMEM((1, rows), jnp.float32),
            pltpu.VMEM((1, rows), jnp.float32),
            pltpu.VMEM((rows, total), jnp.float32),
            pltpu.VMEM((rows, total), jnp.float32),
            pltpu.VMEM((rows, LANES), jnp.float32),
            pltpu.VMEM((rows, LANES), jnp.float32),
            pltpu.VMEM((n, 1, total), jnp.float32),
            pltpu.VMEM((3, lead, total), jnp.float32),
            pltpu.SemaphoreType.DMA((2,)),
            pltpu.SemaphoreType.DMA((PARTS + 1, 2)),
            pltpu.SemaphoreType.DMA((2,)),
            pltpu.SemaphoreType.DMA((3,)),
            pltpu.SemaphoreType.DMA((3,)),
            pltpu.SemaphoreType.DMA((3,)),
            pltpu.SemaphoreType.DMA((n, pieces)),
        ],
        compiler_params=pltpu.CompilerParams(collective_id=0, has_side_effects=True, vmem_limit_bytes=44 * 2**20),
    )(mix_share[None, :], norm_gain[None, :], one_query, other_query, one_key, other_key, one_value, other_value)
    outs = pl.pallas_call(
        functools.partial(store_kernel, widths),
        out_shape=tuple(jax.ShapeDtypeStruct((n, rows, width), jnp.bfloat16) for width in widths)
        + tuple(jax.ShapeDtypeStruct((1, width), jnp.float32) for width in widths),
        in_specs=[vmem, vmem],
        out_specs=(hbm,) * 6,
        scratch_shapes=[pltpu.SemaphoreType.DMA((2, 3))],
        compiler_params=pltpu.CompilerParams(vmem_limit_bytes=2**20),
    )(pltpu.with_memory_space_constraint(buf, pltpu.VMEM), pltpu.with_memory_space_constraint(scale, pltpu.VMEM))
    return tuple(out.reshape(n * rows, -1) for out in outs[:3]) + tuple(out[0] for out in outs[3:])


def solution(mesh):
    n = mesh.shape["shard"]

    def body(*args):
        return routed(n, *args) if fits(n, args[0].shape[0]) else plain(*args)

    return jax.shard_map(
        body,
        mesh=mesh,
        in_specs=(
            P("shard", "width"),
            P("shard", "width"),
            P("shard", "width"),
            P("shard", "width"),
            P("shard", "width"),
            P("shard", "width"),
            P("shard"),
            P("shard"),
        ),
        out_specs=(
            P(None, "width"),
            P(None, "width"),
            P(None, "width"),
            P("width"),
            P("width"),
            P("width"),
        ),
        check_vma=False,
    )
```

```python
import functools
import heapq

import jax
import jax.numpy as jnp
from jax import lax
from jax.experimental import pallas as pl
from jax.experimental.pallas import tpu as pltpu
from jax.sharding import PartitionSpec as P

MESH = pl.DeviceIdType.MESH
ROWS = 16
TILE = 8
LANES = 128
FIRST = ((16, 16, 16, 0), (8, 8, 16, 0))
LEADS = ((48, 48, 32, 32), (16, 16, 16, 16))
UP, DOWN, ACROSS = range(3)
PARTS = 5
FLIGHT = 3
MOST = max(map(max, LEADS))
START = 0


def plain(one_query, other_query, one_key, other_key, one_value, other_value, mix_share, norm_gain):
    result_query = mix_share[:, None] * one_query + (1.0 - mix_share[:, None]) * other_query
    result_key = mix_share[:, None] * one_key + (1.0 - mix_share[:, None]) * other_key
    result_value = mix_share[:, None] * one_value + (1.0 - mix_share[:, None]) * other_value
    result_gained_query = result_query * norm_gain[:, None]
    result_gained_key = result_key * norm_gain[:, None]
    result_gained_value = result_value * norm_gain[:, None]
    total_query, total_key, total_value = lax.psum(
        (
            jnp.sum(result_gained_query * result_gained_query, axis=0),
            jnp.sum(result_gained_key * result_gained_key, axis=0),
            jnp.sum(result_gained_value * result_gained_value, axis=0),
        ),
        "shard",
    )
    scale_query = jnp.sqrt(total_query)
    scale_key = jnp.sqrt(total_key)
    scale_value = jnp.sqrt(total_value)
    narrow_query, narrow_key, narrow_value = (
        (result_gained_query / scale_query).astype(jnp.bfloat16),
        (result_gained_key / scale_key).astype(jnp.bfloat16),
        (result_gained_value / scale_value).astype(jnp.bfloat16),
    )
    final_query, final_key, final_value = (
        lax.all_gather(narrow_query, "shard", axis=0, tiled=True),
        lax.all_gather(narrow_key, "shard", axis=0, tiled=True),
        lax.all_gather(narrow_value, "shard", axis=0, tiled=True),
    )
    return (final_query, final_key, final_value, scale_query, scale_key, scale_value)


def cuts(start, end, parts, unit):
    edges = [start + (end - start) // unit * part // parts * unit for part in range(parts)] + [end]
    return [(low, high - low) for low, high in zip(edges, edges[1:])]


def table(values, z, line):
    return values[z] if z < 2 else values[max(z - line, -2)]


def plan(rows, line, core):
    half = rows // 2 // ROWS * ROWS
    leads = [table(LEADS[core], z, line) for z in range(line)]
    return [[(0, lead)] + cuts(lead, half, 2, ROWS) + [(half, rows - half)] for lead in leads]


def ways_from(z, line):
    return [way for way, ok in ((UP, z < line - 1), (DOWN, z > 0), (ACROSS, True)) if ok]


def early_from(z, line):
    return [way for way, ok in ((UP, z == line - 2), (DOWN, z == 1), (ACROSS, z in (0, line - 1))) if ok]


def relays(line, pieces):
    latency = 3 * TILE
    events, free, serial, order = [], {}, [], [[] for _ in range(line)]

    def send(time, z, way, column, source, c, early=False):
        target = (z + 1, z - 1, z)[way]
        if not early:
            time = free[z, way] = max(time, free.get((z, way), 0)) + pieces[source][c][1]
        serial.append(None)
        heapq.heappush(events, (time + latency * (not early), len(serial), target, column ^ (way == ACROSS), source, c, early))

    def onward(z, column, source, c):
        along = [UP] if (source < z or source == z == 0) and z < line - 1 else []
        along += [DOWN] if (source > z or source == z == line - 1) and z > 0 else []
        crosses = source not in (0, line - 1) or c < len(pieces[source]) - 1
        if column == 0:
            return along + ([ACROSS] if crosses else [])
        return [] if crosses else along

    for z in range(line):
        for way in ways_from(z, line):
            for c in range(len(pieces[z])):
                send(0, z, way, 0, z, c, c == 0 and way in early_from(z, line))
    while events:
        time, _, z, column, source, c, early = heapq.heappop(events)
        ways = onward(z, column, source, c)
        order[z].append((column, source, c, ways, early))
        for way in ways:
            send(time, z, way, column, source, c)
    return order


def sending(level, line, pieces, order):
    early, leaving = early_from(level, line), ways_from(level, line)
    sent = [[sum(size for _, size in pieces[level][way in early:]) if way in leaving else 0, 0] for way in range(3)]
    for _, source, c, ways, _ in order[level]:
        for way in ways:
            sent[way][1] += pieces[source][c][1]
    return sent


def folded(amount, rows, n):
    return next((d for d in range(1, n + 1) if amount % (d * TILE) == 0 and amount // d <= rows), None)


def fits(n, rows):
    if n % 2 or n < 8 or rows % ROWS or rows < 4 * MOST:
        return False
    line = n // 2
    plans = [plan(rows, line, core) for core in range(2)]
    orders = [relays(line, pieces) for pieces in plans]
    return all(folded(amount, rows, n) for pieces, order in zip(plans, orders)
        for z in range(line) for pair in sending(z, line, pieces, order) for amount in pair if amount)


def stages(rows):
    return [(0, MOST)] + cuts(MOST, rows, PARTS, ROWS)


def gather_kernel(n, widths, *refs):
    (share_hbm, gain_hbm), ins, (buf, scale_ref, share_ref, gain_ref, first, second, left, right, sums, pairs, early, row_sem, in_sem, sum_sem, early_send, early_recv, send_sem, recv_sem, token) = refs[:2], refs[2:8], refs[8:]
    rows = first.shape[0]
    total = sum(widths)
    line = n // 2
    me = lax.axis_index("shard")
    z, y = me // 2, me % 2
    other = z * 2 + 1 - y
    core = lax.axis_index("width") % 2
    plans = [plan(rows, line, k) for k in range(2)]
    orders = [relays(line, pieces) for pieces in plans]
    up, down, always = z < line - 1, z > 0, z >= 0
    conditions = (up, down, always)
    targets = (jnp.minimum(z + 1, line - 1) * 2 + y, jnp.maximum(z - 1, 0) * 2 + y, other)
    starts = [sum(widths[:i]) for i in range(len(widths))]

    vectors = [
        pltpu.make_async_copy(source, dest, row_sem.at[i])
        for i, (source, dest) in enumerate(((share_hbm, share_ref), (gain_hbm, gain_ref)))
    ]
    for copy in vectors:
        copy.start()
    parts = stages(rows)

    def load(p):
        low, size = parts[p]
        for i, ref in enumerate(ins):
            dest = (first, second)[i % 2].at[pl.ds(low, size), pl.ds(starts[i // 2], widths[i // 2])]
            pltpu.make_async_copy(ref.at[pl.ds(low, size), :], dest, in_sem.at[p, i % 2]).start()

    def loaded(p):
        for i, ref in enumerate((first, second)):
            whole = ref.at[pl.ds(parts[p][0], parts[p][1]), :]
            pltpu.make_async_copy(whole, whole, in_sem.at[p, i]).wait()

    for p in range(FLIGHT):
        load(p)

    barrier = pltpu.get_barrier_semaphore()
    for way, condition in enumerate(conditions):
        @pl.when(condition)
        def _():
            pl.semaphore_signal(barrier, inc=1, device_id={"shard": targets[way]}, device_id_type=MESH)

    for copy in vectors:
        copy.wait()
    for low in range(0, rows, LANES):
        size = min(LANES, rows - low)
        share, gain = share_ref[:, low:low + size], gain_ref[:, low:low + size]
        for ref, row in ((left, share * gain), (right, (1.0 - share) * gain)):
            ref[pl.ds(low, size), :] = jnp.transpose(jnp.broadcast_to(row, (LANES, size)))

    def mixed(block, acc):
        at = pl.ds(pl.multiple_of(block * ROWS, ROWS), ROWS)
        ours, theirs = (jnp.concatenate([ref[at, :]] * 4, axis=1) for ref in (left, right))
        out = []
        for i in range(len(acc)):
            cols = pl.ds(i * 512, 512)
            value = ours * first[at, cols] + theirs * second[at, cols]
            first[at, cols] = value
            square = value * value
            out.append(acc[i] + square[:8] + square[8:])
        return tuple(out)

    def early_copy(way, low, size):
        return pltpu.make_async_remote_copy(
            src_ref=first.at[pl.ds(low, size), :], dst_ref=early.at[way, pl.ds(low, size), :],
            send_sem=early_send.at[way], recv_sem=early_recv.at[way],
            device_id={"shard": targets[way]}, device_id_type=MESH)

    def start_early(level, ways, low, end):
        for way in ways:
            if way in early_from(level, line) and end > low:
                early_copy(way, low, end - low).start()

    def each_level(act):
        for k in range(2):
            for level in range(line):
                @pl.when((z == level) & (core == k))
                def _():
                    act(level, k)

    def wait_token(level, way):
        if ways_from(level, line).count(1 - way):
            pl.semaphore_wait(token.at[way], 1)

    def send_token(level, way):
        if way in ways_from(level, line):
            pl.semaphore_signal(token.at[way], inc=1, device_id={"shard": targets[way]}, device_id_type=MESH)

    def begun(level, k):
        pl.semaphore_wait(barrier, len(ways_from(level, line)))
        start_early(level, (UP, DOWN, ACROSS), 0, table(FIRST[k], level, line))
        if level == line - 1:
            send_token(level, DOWN)

    def risen(level):
        wait_token(level, UP)
        send_token(level, UP)

    acc = tuple(jnp.zeros((8, 512), jnp.float32) for _ in range(total // 512))
    for p, (low, size) in enumerate(parts):
        loaded(p)
        if p + FLIGHT < len(parts):
            load(p + FLIGHT)
        acc = lax.fori_loop(low // ROWS, (low + size) // ROWS, mixed, acc)
        if p == START:
            each_level(begun)
        for level in range(line):
            if p == min(max(2 * level - 1, 0), len(parts) - 1):
                @pl.when(z == level)
                def _():
                    risen(level)
    for i, value in enumerate(acc):
        sums[me, :, pl.ds(i * 512, 512)] = jnp.sum(value, axis=0, keepdims=True)

    def sum_copy(target, ref, k):
        return pltpu.make_async_remote_copy(
            src_ref=ref, dst_ref=ref, send_sem=sum_sem.at[0], recv_sem=sum_sem.at[k],
            device_id={"shard": target}, device_id_type=MESH)

    def exchanged(level, k):
        first_early, last_early = table(FIRST[k], level, line), plans[k][level][0][1]

        def paired():
            sum_copy(other, sums.at[other], 1).wait_recv()
            pairs[level] = sums[level * 2] + sums[level * 2 + 1]

        def lift(above):
            sum_copy(above * 2 + y, pairs.at[level], 2).start()

        for below in range(level):
            for side in (1 - y, y):
                sum_copy(below * 2 + side, sums.at[me], 2).start()
        sum_copy(other, sums.at[me], 1).start()
        start_early(level, (DOWN, ACROSS), first_early, last_early)
        if level == 0:
            paired()
            lift(1)
        wait_token(level, DOWN)
        if level < line - 1:
            send_token(level, DOWN)
        if level > 0:
            paired()
        for above in range(line - 1, max(level, 1) if level == 0 else level, -1):
            lift(above)
        start_early(level, (UP,), first_early, last_early)
        sum_copy(other, sums.at[pl.ds(0, 2 * (line - 1 - level) + level)], 2).wait_recv()
        for above in range(level + 1, line):
            pairs[above] = sums[above * 2] + sums[above * 2 + 1]
        sum_copy(other, sums.at[pl.ds(0, 2 * level + line - level)], 2).wait_send()

    each_level(exchanged)
    whole = pairs[0]
    for level in range(1, line):
        whole = whole + pairs[level]
    scale = jnp.sqrt(whole)
    scale_ref[...] = scale
    inverse = jnp.broadcast_to(1.0 / scale, (8, total))

    def scaled(source, ref):
        def step(block, carry):
            at = pl.ds(pl.multiple_of(block * ROWS, ROWS), ROWS)
            for i in range(total // 512):
                cols = pl.ds(i * 512, 512)
                wide = jnp.concatenate([inverse[:, i * 512:(i + 1) * 512]] * 2, axis=0)
                buf[source, at, cols] = (ref[at, cols] * wide).astype(buf.dtype)
            return carry
        return step

    def copy(way, source, piece, c, own=False):
        low, size = piece
        ref = buf.at[source, pl.ds(low, size), :]
        return pltpu.make_async_remote_copy(
            src_ref=ref, dst_ref=ref, send_sem=send_sem.at[way, 0 if own else 1], recv_sem=recv_sem.at[source, c],
            device_id={"shard": targets[way]}, device_id_type=MESH)

    def rest(level, k):
        pieces, order = plans[k], orders[k]
        leaving, early_ways = ways_from(level, line), early_from(level, line)

        def scale_rows(source, ref, low, size):
            lax.fori_loop(low // ROWS, (low + size) // ROWS, scaled(source, ref), 0)

        def issue_own(c):
            for way in leaving:
                if c or way not in early_ways:
                    copy(way, me, pieces[level][c], c, True).start()

        for c in (1, 0, 2, 3):
            scale_rows(me, first, *pieces[level][c])
            if c != 1:
                issue_own(1 if c == 0 else 0 if c == 2 else 2)
        issue_own(3)

        came = ((level + 1, DOWN, me + 2), (level - 1, UP, me - 2), (level, ACROSS, other))
        for at, slot, source in came:
            if 0 <= at < line and slot in early_from(at, line):
                piece = pieces[at][0]
                early_copy(slot, *piece).wait_recv()
                scale_rows(source, early.at[slot], *piece)

        for column, at, c, ways, direct in order[level]:
            source = at * 2 + (1 - y if column else y)
            if not direct:
                copy(ACROSS, source, pieces[at][c], c).wait_recv()
            for way in ways:
                copy(way, source, pieces[at][c], c).start()
        amounts = sending(level, line, pieces, order)
        for way, relayed in ((way, relayed) for way in leaving for relayed in range(2)):
            amount = amounts[way][relayed]
            if amount:
                depth = folded(amount, rows, n)
                ref = buf.at[pl.ds(0, depth), pl.ds(0, amount // depth), :]
                pltpu.make_async_remote_copy(
                    src_ref=ref, dst_ref=ref, send_sem=send_sem.at[way, relayed], recv_sem=recv_sem.at[0, 0],
                    device_id={"shard": targets[way]}, device_id_type=MESH).wait_send()
        for way in early_ways:
            early_copy(way, *pieces[level][0]).wait_send()

    each_level(rest)


def store_kernel(widths, buf, scale_ref, *refs):
    outs, scales, sem = refs[:3], refs[3:6], refs[6]
    copies = []
    start = 0
    for i, width in enumerate(widths):
        copies.append(pltpu.make_async_copy(buf.at[:, :, pl.ds(start, width)], outs[i], sem.at[0, i]))
        copies.append(pltpu.make_async_copy(scale_ref.at[:, pl.ds(start, width)], scales[i], sem.at[1, i]))
        start += width
    for copy in copies:
        copy.start()
    for copy in copies:
        copy.wait()


def routed(n, one_query, other_query, one_key, other_key, one_value, other_value, mix_share, norm_gain):
    widths = (one_query.shape[1], one_key.shape[1], one_value.shape[1])
    rows, total = one_query.shape[0], sum(widths)
    pieces = len(plan(rows, n // 2, 0)[0])
    vmem = pl.BlockSpec(memory_space=pltpu.VMEM)
    hbm = pl.BlockSpec(memory_space=pl.ANY)
    buf, scale = pl.pallas_call(
        functools.partial(gather_kernel, n, widths),
        out_shape=(pltpu.VMEM((n, rows, total), jnp.bfloat16), pltpu.VMEM((1, total), jnp.float32)),
        in_specs=[hbm] * 8,
        out_specs=(vmem, vmem),
        scratch_shapes=[
            pltpu.VMEM((1, rows), jnp.float32),
            pltpu.VMEM((1, rows), jnp.float32),
            pltpu.VMEM((rows, total), jnp.float32),
            pltpu.VMEM((rows, total), jnp.float32),
            pltpu.VMEM((rows, LANES), jnp.float32),
            pltpu.VMEM((rows, LANES), jnp.float32),
            pltpu.VMEM((n, 1, total), jnp.float32),
            pltpu.VMEM((n // 2, 1, total), jnp.float32),
            pltpu.VMEM((3, MOST, total), jnp.float32),
            pltpu.SemaphoreType.DMA((2,)),
            pltpu.SemaphoreType.DMA((PARTS + 1, 2)),
            pltpu.SemaphoreType.DMA((3,)),
            pltpu.SemaphoreType.DMA((3,)),
            pltpu.SemaphoreType.DMA((3,)),
            pltpu.SemaphoreType.DMA((3, 2)),
            pltpu.SemaphoreType.DMA((n, pieces)),
            pltpu.SemaphoreType.REGULAR((2,)),
        ],
        compiler_params=pltpu.CompilerParams(collective_id=0, has_side_effects=True, vmem_limit_bytes=44 * 2**20),
    )(mix_share[None, :], norm_gain[None, :], one_query, other_query, one_key, other_key, one_value, other_value)
    outs = pl.pallas_call(
        functools.partial(store_kernel, widths),
        out_shape=tuple(jax.ShapeDtypeStruct((n, rows, width), jnp.bfloat16) for width in widths)
        + tuple(jax.ShapeDtypeStruct((1, width), jnp.float32) for width in widths),
        in_specs=[vmem, vmem],
        out_specs=(hbm,) * 6,
        scratch_shapes=[pltpu.SemaphoreType.DMA((2, 3))],
        compiler_params=pltpu.CompilerParams(vmem_limit_bytes=2**20),
    )(pltpu.with_memory_space_constraint(buf, pltpu.VMEM), pltpu.with_memory_space_constraint(scale, pltpu.VMEM))
    return tuple(out.reshape(n * rows, -1) for out in outs[:3]) + tuple(out[0] for out in outs[3:])


def solution(mesh):
    n = mesh.shape["shard"]

    def body(*args):
        return routed(n, *args) if fits(n, args[0].shape[0]) else plain(*args)

    return jax.shard_map(
        body,
        mesh=mesh,
        in_specs=(
            P("shard", "width"),
            P("shard", "width"),
            P("shard", "width"),
            P("shard", "width"),
            P("shard", "width"),
            P("shard", "width"),
            P("shard"),
            P("shard"),
        ),
        out_specs=(
            P(None, "width"),
            P(None, "width"),
            P(None, "width"),
            P("width"),
            P("width"),
            P("width"),
        ),
        check_vma=False,
    )
```

```python
import functools
import heapq

import jax
import jax.numpy as jnp
from jax import lax
from jax.experimental import pallas as pl
from jax.experimental.pallas import tpu as pltpu
from jax.sharding import PartitionSpec as P

MESH = pl.DeviceIdType.MESH
ROWS = 16
TILE = 8
LANES = 128
FIRST = ((16, 16, 16, 0), (16, 16, 16, 0))
LEADS = ((32, 32, 32, 16), (32, 32, 16, 16))
UP, DOWN, ACROSS = range(3)
PARTS = 5
FLIGHT = 3
MOST = max(map(max, LEADS))
START = 0


def plain(one_query, other_query, one_key, other_key, one_value, other_value, mix_share, norm_gain):
    result_query = mix_share[:, None] * one_query + (1.0 - mix_share[:, None]) * other_query
    result_key = mix_share[:, None] * one_key + (1.0 - mix_share[:, None]) * other_key
    result_value = mix_share[:, None] * one_value + (1.0 - mix_share[:, None]) * other_value
    result_gained_query = result_query * norm_gain[:, None]
    result_gained_key = result_key * norm_gain[:, None]
    result_gained_value = result_value * norm_gain[:, None]
    total_query, total_key, total_value = lax.psum(
        (
            jnp.sum(result_gained_query * result_gained_query, axis=0),
            jnp.sum(result_gained_key * result_gained_key, axis=0),
            jnp.sum(result_gained_value * result_gained_value, axis=0),
        ),
        "shard",
    )
    scale_query = jnp.sqrt(total_query)
    scale_key = jnp.sqrt(total_key)
    scale_value = jnp.sqrt(total_value)
    narrow_query, narrow_key, narrow_value = (
        (result_gained_query / scale_query).astype(jnp.bfloat16),
        (result_gained_key / scale_key).astype(jnp.bfloat16),
        (result_gained_value / scale_value).astype(jnp.bfloat16),
    )
    final_query, final_key, final_value = (
        lax.all_gather(narrow_query, "shard", axis=0, tiled=True),
        lax.all_gather(narrow_key, "shard", axis=0, tiled=True),
        lax.all_gather(narrow_value, "shard", axis=0, tiled=True),
    )
    return (final_query, final_key, final_value, scale_query, scale_key, scale_value)


def cuts(start, end, parts, unit):
    edges = [start + (end - start) // unit * part // parts * unit for part in range(parts)] + [end]
    return [(low, high - low) for low, high in zip(edges, edges[1:])]


def table(values, z, line):
    return values[z] if z < 2 else values[max(z - line, -2)]


def plan(rows, line, core):
    half = rows // 2 // ROWS * ROWS
    leads = [table(LEADS[core], z, line) for z in range(line)]
    return [[(0, lead)] + cuts(lead, half, 2, ROWS) + [(half, rows - half)] for lead in leads]


def ways_from(z, line):
    return [way for way, ok in ((UP, z < line - 1), (DOWN, z > 0), (ACROSS, True)) if ok]


def early_from(z, line):
    return [way for way, ok in ((UP, z == line - 2), (DOWN, z == 1), (ACROSS, z in (0, line - 1))) if ok]


def relays(line, pieces):
    latency = 3 * TILE
    events, free, serial, order = [], {}, [], [[] for _ in range(line)]

    def send(time, z, way, column, source, c, early=False):
        target = (z + 1, z - 1, z)[way]
        if not early:
            time = free[z, way] = max(time, free.get((z, way), 0)) + pieces[source][c][1]
        serial.append(None)
        heapq.heappush(events, (time + latency * (not early), len(serial), target, column ^ (way == ACROSS), source, c, early))

    def onward(z, column, source, c):
        along = [UP] if (source < z or source == z == 0) and z < line - 1 else []
        along += [DOWN] if (source > z or source == z == line - 1) and z > 0 else []
        crosses = source not in (0, line - 1) or c < len(pieces[source]) - 1
        if column == 0:
            return along + ([ACROSS] if crosses else [])
        return [] if crosses else along

    for z in range(line):
        for way in ways_from(z, line):
            for c in range(len(pieces[z])):
                send(0, z, way, 0, z, c, c == 0 and way in early_from(z, line))
    while events:
        time, _, z, column, source, c, early = heapq.heappop(events)
        ways = onward(z, column, source, c)
        order[z].append((column, source, c, ways, early))
        for way in ways:
            send(time, z, way, column, source, c)
    return order


def sending(level, line, pieces, order):
    early, leaving = early_from(level, line), ways_from(level, line)
    sent = [[sum(size for _, size in pieces[level][way in early:]) if way in leaving else 0, 0] for way in range(3)]
    for _, source, c, ways, _ in order[level]:
        for way in ways:
            sent[way][1] += pieces[source][c][1]
    return sent


def folded(amount, rows, n):
    return next((d for d in range(1, n + 1) if amount % (d * TILE) == 0 and amount // d <= rows), None)


def fits(n, rows):
    if n % 2 or n < 8 or rows % ROWS or rows < 4 * MOST:
        return False
    line = n // 2
    plans = [plan(rows, line, core) for core in range(2)]
    orders = [relays(line, pieces) for pieces in plans]
    return all(folded(amount, rows, n) for pieces, order in zip(plans, orders)
        for z in range(line) for pair in sending(z, line, pieces, order) for amount in pair if amount)


def stages(rows):
    return [(0, MOST)] + cuts(MOST, rows, PARTS, ROWS)


def gather_kernel(n, widths, *refs):
    (share_hbm, gain_hbm), ins, (buf, scale_ref, share_ref, gain_ref, first, second, left, right, sums, pairs, early, row_sem, in_sem, sum_sem, early_send, early_recv, send_sem, recv_sem, token) = refs[:2], refs[2:8], refs[8:]
    rows = first.shape[0]
    total = sum(widths)
    line = n // 2
    me = lax.axis_index("shard")
    z, y = me // 2, me % 2
    other = z * 2 + 1 - y
    core = lax.axis_index("width") % 2
    plans = [plan(rows, line, k) for k in range(2)]
    orders = [relays(line, pieces) for pieces in plans]
    up, down, always = z < line - 1, z > 0, z >= 0
    conditions = (up, down, always)
    targets = (jnp.minimum(z + 1, line - 1) * 2 + y, jnp.maximum(z - 1, 0) * 2 + y, other)
    starts = [sum(widths[:i]) for i in range(len(widths))]

    vectors = [
        pltpu.make_async_copy(source, dest, row_sem.at[i])
        for i, (source, dest) in enumerate(((share_hbm, share_ref), (gain_hbm, gain_ref)))
    ]
    for copy in vectors:
        copy.start()
    parts = stages(rows)

    def load(p):
        low, size = parts[p]
        for i, ref in enumerate(ins):
            dest = (first, second)[i % 2].at[pl.ds(low, size), pl.ds(starts[i // 2], widths[i // 2])]
            pltpu.make_async_copy(ref.at[pl.ds(low, size), :], dest, in_sem.at[p, i % 2]).start()

    def loaded(p):
        for i, ref in enumerate((first, second)):
            whole = ref.at[pl.ds(parts[p][0], parts[p][1]), :]
            pltpu.make_async_copy(whole, whole, in_sem.at[p, i]).wait()

    load(0)

    barrier = pltpu.get_barrier_semaphore()
    for way, condition in enumerate(conditions):
        @pl.when(condition)
        def _():
            pl.semaphore_signal(barrier, inc=1, device_id={"shard": targets[way]}, device_id_type=MESH)

    for p in range(1, len(parts)):
        load(p)

    for copy in vectors:
        copy.wait()
    for low in range(0, rows, LANES):
        size = min(LANES, rows - low)
        share, gain = share_ref[:, low:low + size], gain_ref[:, low:low + size]
        for ref, row in ((left, share * gain), (right, (1.0 - share) * gain)):
            ref[pl.ds(low, size), :] = jnp.transpose(jnp.broadcast_to(row, (LANES, size)))

    def mixed(block, acc):
        at = pl.ds(pl.multiple_of(block * ROWS, ROWS), ROWS)
        ours, theirs = (jnp.concatenate([ref[at, :]] * 4, axis=1) for ref in (left, right))
        out = []
        for i in range(len(acc)):
            cols = pl.ds(i * 512, 512)
            value = ours * first[at, cols] + theirs * second[at, cols]
            first[at, cols] = value
            square = value * value
            out.append(acc[i] + square[:8] + square[8:])
        return tuple(out)

    def early_copy(way, low, size):
        return pltpu.make_async_remote_copy(
            src_ref=first.at[pl.ds(low, size), :], dst_ref=early.at[way, pl.ds(low, size), :],
            send_sem=early_send.at[way], recv_sem=early_recv.at[way],
            device_id={"shard": targets[way]}, device_id_type=MESH)

    def start_early(level, ways, low, end):
        for way in ways:
            if way in early_from(level, line) and end > low:
                early_copy(way, low, end - low).start()

    def each_level(act):
        for k in range(2):
            for level in range(line):
                @pl.when((z == level) & (core == k))
                def _():
                    act(level, k)

    def wait_token(level, way):
        if ways_from(level, line).count(1 - way):
            pl.semaphore_wait(token.at[way], 1)

    def send_token(level, way):
        if way in ways_from(level, line):
            pl.semaphore_signal(token.at[way], inc=1, device_id={"shard": targets[way]}, device_id_type=MESH)

    def begun(level, k):
        pl.semaphore_wait(barrier, len(ways_from(level, line)))
        start_early(level, (UP, DOWN, ACROSS), 0, table(FIRST[k], level, line))
        if level == line - 1:
            send_token(level, DOWN)

    def risen(level):
        wait_token(level, UP)
        send_token(level, UP)

    acc = tuple(jnp.zeros((8, 512), jnp.float32) for _ in range(total // 512))
    for p, (low, size) in enumerate(parts):
        loaded(p)
        acc = lax.fori_loop(low // ROWS, (low + size) // ROWS, mixed, acc)
        if p == START:
            each_level(begun)
        for level in range(line):
            if p == min(max(2 * level - 1, 0), len(parts) - 1):
                @pl.when(z == level)
                def _():
                    risen(level)
    for i, value in enumerate(acc):
        sums[me, :, pl.ds(i * 512, 512)] = jnp.sum(value, axis=0, keepdims=True)

    def sum_copy(target, ref, k):
        return pltpu.make_async_remote_copy(
            src_ref=ref, dst_ref=ref, send_sem=sum_sem.at[0], recv_sem=sum_sem.at[k],
            device_id={"shard": target}, device_id_type=MESH)

    def exchanged(level, k):
        first_early, last_early = table(FIRST[k], level, line), plans[k][level][0][1]

        def paired():
            sum_copy(other, sums.at[other], 1).wait_recv()
            pairs[level] = sums[level * 2] + sums[level * 2 + 1]

        def lift(above):
            sum_copy(above * 2 + y, pairs.at[level], 2).start()

        for below in range(level):
            for side in (1 - y, y):
                sum_copy(below * 2 + side, sums.at[me], 2).start()
        sum_copy(other, sums.at[me], 1).start()
        start_early(level, (DOWN, ACROSS), first_early, last_early)
        if level == 0:
            paired()
            lift(1)
        wait_token(level, DOWN)
        if level < line - 1:
            send_token(level, DOWN)
        if level > 0:
            paired()
        for above in range(line - 1, max(level, 1) if level == 0 else level, -1):
            lift(above)
        start_early(level, (UP,), first_early, last_early)
        sum_copy(other, sums.at[pl.ds(0, 2 * (line - 1 - level) + level)], 2).wait_recv()
        for above in range(level + 1, line):
            pairs[above] = sums[above * 2] + sums[above * 2 + 1]
        sum_copy(other, sums.at[pl.ds(0, 2 * level + line - level)], 2).wait_send()

    each_level(exchanged)
    whole = pairs[0]
    for level in range(1, line):
        whole = whole + pairs[level]
    scale = jnp.sqrt(whole)
    scale_ref[...] = scale
    inverse = jnp.broadcast_to(1.0 / scale, (8, total))

    def scaled(source, ref):
        def step(block, carry):
            at = pl.ds(pl.multiple_of(block * ROWS, ROWS), ROWS)
            for i in range(total // 512):
                cols = pl.ds(i * 512, 512)
                wide = jnp.concatenate([inverse[:, i * 512:(i + 1) * 512]] * 2, axis=0)
                buf[source, at, cols] = (ref[at, cols] * wide).astype(buf.dtype)
            return carry
        return step

    def copy(way, source, piece, c, own=False):
        low, size = piece
        ref = buf.at[source, pl.ds(low, size), :]
        return pltpu.make_async_remote_copy(
            src_ref=ref, dst_ref=ref, send_sem=send_sem.at[way, 0 if own else 1], recv_sem=recv_sem.at[source, c],
            device_id={"shard": targets[way]}, device_id_type=MESH)

    def rest(level, k):
        pieces, order = plans[k], orders[k]
        leaving, early_ways = ways_from(level, line), early_from(level, line)

        def scale_rows(source, ref, low, size):
            lax.fori_loop(low // ROWS, (low + size) // ROWS, scaled(source, ref), 0)

        def issue_own(c):
            for way in leaving:
                if c or way not in early_ways:
                    copy(way, me, pieces[level][c], c, True).start()

        for c in (1, 0, 2, 3):
            scale_rows(me, first, *pieces[level][c])
            if c != 1:
                issue_own(1 if c == 0 else 0 if c == 2 else 2)
        issue_own(3)

        came = ((level + 1, DOWN, me + 2), (level - 1, UP, me - 2), (level, ACROSS, other))
        for at, slot, source in came:
            if 0 <= at < line and slot in early_from(at, line):
                piece = pieces[at][0]
                early_copy(slot, *piece).wait_recv()
                scale_rows(source, early.at[slot], *piece)

        for column, at, c, ways, direct in order[level]:
            source = at * 2 + (1 - y if column else y)
            if not direct:
                copy(ACROSS, source, pieces[at][c], c).wait_recv()
            for way in ways:
                copy(way, source, pieces[at][c], c).start()
        amounts = sending(level, line, pieces, order)
        for way, relayed in ((way, relayed) for way in leaving for relayed in range(2)):
            amount = amounts[way][relayed]
            if amount:
                depth = folded(amount, rows, n)
                ref = buf.at[pl.ds(0, depth), pl.ds(0, amount // depth), :]
                pltpu.make_async_remote_copy(
                    src_ref=ref, dst_ref=ref, send_sem=send_sem.at[way, relayed], recv_sem=recv_sem.at[0, 0],
                    device_id={"shard": targets[way]}, device_id_type=MESH).wait_send()
        for way in early_ways:
            early_copy(way, *pieces[level][0]).wait_send()

    each_level(rest)


def store_kernel(widths, buf, scale_ref, *refs):
    outs, scales, sem = refs[:3], refs[3:6], refs[6]
    copies = []
    start = 0
    for i, width in enumerate(widths):
        copies.append(pltpu.make_async_copy(buf.at[:, :, pl.ds(start, width)], outs[i], sem.at[0, i]))
        copies.append(pltpu.make_async_copy(scale_ref.at[:, pl.ds(start, width)], scales[i], sem.at[1, i]))
        start += width
    for copy in copies:
        copy.start()
    for copy in copies:
        copy.wait()


def routed(n, one_query, other_query, one_key, other_key, one_value, other_value, mix_share, norm_gain):
    widths = (one_query.shape[1], one_key.shape[1], one_value.shape[1])
    rows, total = one_query.shape[0], sum(widths)
    pieces = len(plan(rows, n // 2, 0)[0])
    vmem = pl.BlockSpec(memory_space=pltpu.VMEM)
    hbm = pl.BlockSpec(memory_space=pl.ANY)
    buf, scale = pl.pallas_call(
        functools.partial(gather_kernel, n, widths),
        out_shape=(pltpu.VMEM((n, rows, total), jnp.bfloat16), pltpu.VMEM((1, total), jnp.float32)),
        in_specs=[hbm] * 8,
        out_specs=(vmem, vmem),
        scratch_shapes=[
            pltpu.VMEM((1, rows), jnp.float32),
            pltpu.VMEM((1, rows), jnp.float32),
            pltpu.VMEM((rows, total), jnp.float32),
            pltpu.VMEM((rows, total), jnp.float32),
            pltpu.VMEM((rows, LANES), jnp.float32),
            pltpu.VMEM((rows, LANES), jnp.float32),
            pltpu.VMEM((n, 1, total), jnp.float32),
            pltpu.VMEM((n // 2, 1, total), jnp.float32),
            pltpu.VMEM((3, MOST, total), jnp.float32),
            pltpu.SemaphoreType.DMA((2,)),
            pltpu.SemaphoreType.DMA((PARTS + 1, 2)),
            pltpu.SemaphoreType.DMA((3,)),
            pltpu.SemaphoreType.DMA((3,)),
            pltpu.SemaphoreType.DMA((3,)),
            pltpu.SemaphoreType.DMA((3, 2)),
            pltpu.SemaphoreType.DMA((n, pieces)),
            pltpu.SemaphoreType.REGULAR((2,)),
        ],
        compiler_params=pltpu.CompilerParams(collective_id=0, has_side_effects=True, vmem_limit_bytes=44 * 2**20),
    )(mix_share[None, :], norm_gain[None, :], one_query, other_query, one_key, other_key, one_value, other_value)
    outs = pl.pallas_call(
        functools.partial(store_kernel, widths),
        out_shape=tuple(jax.ShapeDtypeStruct((n, rows, width), jnp.bfloat16) for width in widths)
        + tuple(jax.ShapeDtypeStruct((1, width), jnp.float32) for width in widths),
        in_specs=[vmem, vmem],
        out_specs=(hbm,) * 6,
        scratch_shapes=[pltpu.SemaphoreType.DMA((2, 3))],
        compiler_params=pltpu.CompilerParams(vmem_limit_bytes=2**20),
    )(pltpu.with_memory_space_constraint(buf, pltpu.VMEM), pltpu.with_memory_space_constraint(scale, pltpu.VMEM))
    return tuple(out.reshape(n * rows, -1) for out in outs[:3]) + tuple(out[0] for out in outs[3:])


def solution(mesh):
    n = mesh.shape["shard"]

    def body(*args):
        return routed(n, *args) if fits(n, args[0].shape[0]) else plain(*args)

    return jax.shard_map(
        body,
        mesh=mesh,
        in_specs=(
            P("shard", "width"),
            P("shard", "width"),
            P("shard", "width"),
            P("shard", "width"),
            P("shard", "width"),
            P("shard", "width"),
            P("shard"),
            P("shard"),
        ),
        out_specs=(
            P(None, "width"),
            P(None, "width"),
            P(None, "width"),
            P("width"),
            P("width"),
            P("width"),
        ),
        check_vma=False,
    )
```

```python
import functools
import heapq

import jax
import jax.numpy as jnp
from jax import lax
from jax.experimental import pallas as pl
from jax.experimental.pallas import tpu as pltpu
from jax.sharding import PartitionSpec as P

MESH = pl.DeviceIdType.MESH
ROWS = 16
TILE = 8
LANES = 128
FIRST = ((16, 16, 16, 0), (16, 16, 16, 0))
LEADS = ((32, 32, 32, 16), (32, 32, 16, 16))
UP, DOWN, ACROSS = range(3)
PARTS = 5
FLIGHT = 3
MOST = max(map(max, LEADS))
START = 0
GAPS = ((0, 0), (2, 1))


def plain(one_query, other_query, one_key, other_key, one_value, other_value, mix_share, norm_gain):
    result_query = mix_share[:, None] * one_query + (1.0 - mix_share[:, None]) * other_query
    result_key = mix_share[:, None] * one_key + (1.0 - mix_share[:, None]) * other_key
    result_value = mix_share[:, None] * one_value + (1.0 - mix_share[:, None]) * other_value
    result_gained_query = result_query * norm_gain[:, None]
    result_gained_key = result_key * norm_gain[:, None]
    result_gained_value = result_value * norm_gain[:, None]
    total_query, total_key, total_value = lax.psum(
        (
            jnp.sum(result_gained_query * result_gained_query, axis=0),
            jnp.sum(result_gained_key * result_gained_key, axis=0),
            jnp.sum(result_gained_value * result_gained_value, axis=0),
        ),
        "shard",
    )
    scale_query = jnp.sqrt(total_query)
    scale_key = jnp.sqrt(total_key)
    scale_value = jnp.sqrt(total_value)
    narrow_query, narrow_key, narrow_value = (
        (result_gained_query / scale_query).astype(jnp.bfloat16),
        (result_gained_key / scale_key).astype(jnp.bfloat16),
        (result_gained_value / scale_value).astype(jnp.bfloat16),
    )
    final_query, final_key, final_value = (
        lax.all_gather(narrow_query, "shard", axis=0, tiled=True),
        lax.all_gather(narrow_key, "shard", axis=0, tiled=True),
        lax.all_gather(narrow_value, "shard", axis=0, tiled=True),
    )
    return (final_query, final_key, final_value, scale_query, scale_key, scale_value)


def cuts(start, end, parts, unit):
    edges = [start + (end - start) // unit * part // parts * unit for part in range(parts)] + [end]
    return [(low, high - low) for low, high in zip(edges, edges[1:])]


def table(values, z, line):
    return values[z] if z < 2 else values[max(z - line, -2)]


def plan(rows, line, core):
    half = rows // 2 // ROWS * ROWS
    leads = [table(LEADS[core], z, line) for z in range(line)]
    return [[(0, lead)] + cuts(lead, half, 2, ROWS) + [(half, rows - half)] for lead in leads]


def ways_from(z, line):
    return [way for way, ok in ((UP, z < line - 1), (DOWN, z > 0), (ACROSS, True)) if ok]


def early_from(z, line):
    return [way for way, ok in ((UP, z == line - 2), (DOWN, z == 1), (ACROSS, z in (0, line - 1))) if ok]


def relays(line, pieces):
    latency = 3 * TILE
    events, free, serial, order = [], {}, [], [[] for _ in range(line)]

    def send(time, z, way, column, source, c, early=False):
        target = (z + 1, z - 1, z)[way]
        if not early:
            time = free[z, way] = max(time, free.get((z, way), 0)) + pieces[source][c][1]
        serial.append(None)
        heapq.heappush(events, (time + latency * (not early), len(serial), target, column ^ (way == ACROSS), source, c, early))

    def onward(z, column, source, c):
        along = [UP] if (source < z or source == z == 0) and z < line - 1 else []
        along += [DOWN] if (source > z or source == z == line - 1) and z > 0 else []
        crosses = source not in (0, line - 1) or c < len(pieces[source]) - 1
        if column == 0:
            return along + ([ACROSS] if crosses else [])
        return [] if crosses else along

    for z in range(line):
        for way in ways_from(z, line):
            for c in range(len(pieces[z])):
                send(0, z, way, 0, z, c, c == 0 and way in early_from(z, line))
    while events:
        time, _, z, column, source, c, early = heapq.heappop(events)
        ways = onward(z, column, source, c)
        order[z].append((column, source, c, ways, early))
        for way in ways:
            send(time, z, way, column, source, c)
    return order


def sending(level, line, pieces, order):
    early, leaving = early_from(level, line), ways_from(level, line)
    sent = [[sum(size for _, size in pieces[level][way in early:]) if way in leaving else 0, 0] for way in range(3)]
    for _, source, c, ways, _ in order[level]:
        for way in ways:
            sent[way][1] += pieces[source][c][1]
    return sent


def folded(amount, rows, n):
    return next((d for d in range(1, n + 1) if amount % (d * TILE) == 0 and amount // d <= rows), None)


def fits(n, rows):
    if n % 2 or n < 8 or rows % ROWS or rows < 4 * MOST:
        return False
    line = n // 2
    plans = [plan(rows, line, core) for core in range(2)]
    orders = [relays(line, pieces) for pieces in plans]
    return all(folded(amount, rows, n) for pieces, order in zip(plans, orders)
        for z in range(line) for pair in sending(z, line, pieces, order) for amount in pair if amount)


def stages(rows):
    return [(0, MOST)] + cuts(MOST, rows, PARTS, ROWS)


def gather_kernel(n, widths, *refs):
    (share_hbm, gain_hbm), ins, (buf, scale_ref, share_ref, gain_ref, first, second, left, right, sums, pairs, early, row_sem, in_sem, sum_sem, early_send, early_recv, send_sem, recv_sem, token) = refs[:2], refs[2:8], refs[8:]
    rows = first.shape[0]
    total = sum(widths)
    line = n // 2
    me = lax.axis_index("shard")
    z, y = me // 2, me % 2
    other = z * 2 + 1 - y
    core = lax.axis_index("width") % 2
    plans = [plan(rows, line, k) for k in range(2)]
    orders = [relays(line, pieces) for pieces in plans]
    up, down, always = z < line - 1, z > 0, z >= 0
    conditions = (up, down, always)
    targets = (jnp.minimum(z + 1, line - 1) * 2 + y, jnp.maximum(z - 1, 0) * 2 + y, other)
    starts = [sum(widths[:i]) for i in range(len(widths))]

    vectors = [
        pltpu.make_async_copy(source, dest, row_sem.at[i])
        for i, (source, dest) in enumerate(((share_hbm, share_ref), (gain_hbm, gain_ref)))
    ]
    for copy in vectors:
        copy.start()
    parts = stages(rows)

    def load(p):
        low, size = parts[p]
        for i, ref in enumerate(ins):
            dest = (first, second)[i % 2].at[pl.ds(low, size), pl.ds(starts[i // 2], widths[i // 2])]
            pltpu.make_async_copy(ref.at[pl.ds(low, size), :], dest, in_sem.at[p, i % 2]).start()

    def loaded(p):
        for i, ref in enumerate((first, second)):
            whole = ref.at[pl.ds(parts[p][0], parts[p][1]), :]
            pltpu.make_async_copy(whole, whole, in_sem.at[p, i]).wait()

    load(0)

    barrier = pltpu.get_barrier_semaphore()
    for way, condition in enumerate(conditions):
        @pl.when(condition)
        def _():
            pl.semaphore_signal(barrier, inc=1, device_id={"shard": targets[way]}, device_id_type=MESH)

    for p in range(1, len(parts)):
        load(p)

    for copy in vectors:
        copy.wait()
    for low in range(0, rows, LANES):
        size = min(LANES, rows - low)
        share, gain = share_ref[:, low:low + size], gain_ref[:, low:low + size]
        for ref, row in ((left, share * gain), (right, (1.0 - share) * gain)):
            ref[pl.ds(low, size), :] = jnp.transpose(jnp.broadcast_to(row, (LANES, size)))

    def mixed(block, acc):
        at = pl.ds(pl.multiple_of(block * ROWS, ROWS), ROWS)
        ours, theirs = (jnp.concatenate([ref[at, :]] * 4, axis=1) for ref in (left, right))
        out = []
        for i in range(len(acc)):
            cols = pl.ds(i * 512, 512)
            value = ours * first[at, cols] + theirs * second[at, cols]
            first[at, cols] = value
            square = value * value
            out.append(acc[i] + square[:8] + square[8:])
        return tuple(out)

    def early_copy(way, low, size):
        return pltpu.make_async_remote_copy(
            src_ref=first.at[pl.ds(low, size), :], dst_ref=early.at[way, pl.ds(low, size), :],
            send_sem=early_send.at[way], recv_sem=early_recv.at[way],
            device_id={"shard": targets[way]}, device_id_type=MESH)

    def start_early(level, ways, low, end):
        for way in ways:
            if way in early_from(level, line) and end > low:
                early_copy(way, low, end - low).start()

    def each_level(act):
        for k in range(2):
            for level in range(line):
                @pl.when((z == level) & (core == k))
                def _():
                    act(level, k)

    def wait_token(level, way):
        if ways_from(level, line).count(1 - way):
            pl.semaphore_wait(token.at[way], 1)

    def send_token(level, way):
        if way in ways_from(level, line):
            pl.semaphore_signal(token.at[way], inc=1, device_id={"shard": targets[way]}, device_id_type=MESH)

    def begun(level, k):
        pl.semaphore_wait(barrier, len(ways_from(level, line)))
        start_early(level, (UP, DOWN, ACROSS), 0, table(FIRST[k], level, line))
        if level == line - 1:
            send_token(level, DOWN)

    def risen(level):
        wait_token(level, UP)
        send_token(level, UP)

    acc = tuple(jnp.zeros((8, 512), jnp.float32) for _ in range(total // 512))
    for p, (low, size) in enumerate(parts):
        loaded(p)
        acc = lax.fori_loop(low // ROWS, (low + size) // ROWS, mixed, acc)
        if p == START:
            each_level(begun)
        for level in range(line):
            if p == min(max(2 * level - 1, 0), len(parts) - 1):
                @pl.when(z == level)
                def _():
                    risen(level)
    for i, value in enumerate(acc):
        sums[me, :, pl.ds(i * 512, 512)] = jnp.sum(value, axis=0, keepdims=True)

    def sum_copy(target, ref, k):
        return pltpu.make_async_remote_copy(
            src_ref=ref, dst_ref=ref, send_sem=sum_sem.at[0], recv_sem=sum_sem.at[k],
            device_id={"shard": target}, device_id_type=MESH)

    def exchanged(level, k):
        first_early, last_early = table(FIRST[k], level, line), plans[k][level][0][1]

        def paired():
            sum_copy(other, sums.at[other], 1).wait_recv()
            pairs[level] = sums[level * 2] + sums[level * 2 + 1]

        def lift(above):
            sum_copy(above * 2 + y, pairs.at[level], 2).start()

        for below in range(level):
            for side in (1 - y, y):
                sum_copy(below * 2 + side, sums.at[me], 2).start()
        sum_copy(other, sums.at[me], 1).start()
        start_early(level, (DOWN, ACROSS), first_early, last_early)
        if level == 0:
            paired()
            lift(1)
        wait_token(level, DOWN)
        if level < line - 1:
            send_token(level, DOWN)
        if level > 0:
            paired()
        for above in range(line - 1, max(level, 1) if level == 0 else level, -1):
            lift(above)
        start_early(level, (UP,), first_early, last_early)
        sum_copy(other, sums.at[pl.ds(0, 2 * (line - 1 - level) + level)], 2).wait_recv()
        for above in range(level + 1, line):
            pairs[above] = sums[above * 2] + sums[above * 2 + 1]
        sum_copy(other, sums.at[pl.ds(0, 2 * level + line - level)], 2).wait_send()

    each_level(exchanged)
    whole = pairs[0]
    for level in range(1, line):
        whole = whole + pairs[level]
    scale = jnp.sqrt(whole)
    scale_ref[...] = scale
    inverse = jnp.broadcast_to(1.0 / scale, (8, total))

    def scaled(source, ref):
        def step(block, carry):
            at = pl.ds(pl.multiple_of(block * ROWS, ROWS), ROWS)
            for i in range(total // 512):
                cols = pl.ds(i * 512, 512)
                wide = jnp.concatenate([inverse[:, i * 512:(i + 1) * 512]] * 2, axis=0)
                buf[source, at, cols] = (ref[at, cols] * wide).astype(buf.dtype)
            return carry
        return step

    def copy(way, source, piece, c, own=False):
        low, size = piece
        ref = buf.at[source, pl.ds(low, size), :]
        return pltpu.make_async_remote_copy(
            src_ref=ref, dst_ref=ref, send_sem=send_sem.at[way, 0 if own else 1], recv_sem=recv_sem.at[source, c],
            device_id={"shard": targets[way]}, device_id_type=MESH)

    def rest(level, k):
        pieces, order = plans[k], orders[k]
        leaving, early_ways = ways_from(level, line), early_from(level, line)

        def scale_rows(source, ref, low, size):
            lax.fori_loop(low // ROWS, (low + size) // ROWS, scaled(source, ref), 0)

        gaps = GAPS[k][level] if level < 2 else 0
        last = len(pieces[level]) - 1
        events = [(1, level, last - 1), (1, level, last)][:gaps]
        held = []

        def issue_own(c):
            for way in leaving:
                if c == last and way in early_ways and gaps:
                    held.append((way, me, pieces[level][c], c, True))
                elif c or way not in early_ways:
                    copy(way, me, pieces[level][c], c, True).start()

        for c in (1, 0, 2, 3):
            scale_rows(me, first, *pieces[level][c])
            if c != 1:
                issue_own(1 if c == 0 else 0 if c == 2 else 2)
        issue_own(last)

        came = ((level + 1, DOWN, me + 2), (level - 1, UP, me - 2), (level, ACROSS, other))
        for at, slot, source in came:
            if 0 <= at < line and slot in early_from(at, line):
                piece = pieces[at][0]
                early_copy(slot, *piece).wait_recv()
                scale_rows(source, early.at[slot], *piece)

        for column, at, c, ways, direct in order[level]:
            source = at * 2 + (1 - y if column else y)
            if not direct:
                copy(ACROSS, source, pieces[at][c], c).wait_recv()
            for way in ways:
                if events and way in early_ways:
                    held.append((way, source, pieces[at][c], c))
                else:
                    copy(way, source, pieces[at][c], c).start()
            if events and (column, at, c) == events[0]:
                events.pop(0)
                ready = 1 if events else len(held)
                for args in held[:ready]:
                    copy(*args).start()
                del held[:ready]
        amounts = sending(level, line, pieces, order)
        for way, relayed in ((way, relayed) for way in leaving for relayed in range(2)):
            amount = amounts[way][relayed]
            if amount:
                depth = folded(amount, rows, n)
                ref = buf.at[pl.ds(0, depth), pl.ds(0, amount // depth), :]
                pltpu.make_async_remote_copy(
                    src_ref=ref, dst_ref=ref, send_sem=send_sem.at[way, relayed], recv_sem=recv_sem.at[0, 0],
                    device_id={"shard": targets[way]}, device_id_type=MESH).wait_send()
        for way in early_ways:
            early_copy(way, *pieces[level][0]).wait_send()

    each_level(rest)


def store_kernel(widths, buf, scale_ref, *refs):
    outs, scales, sem = refs[:3], refs[3:6], refs[6]
    copies = []
    start = 0
    for i, width in enumerate(widths):
        copies.append(pltpu.make_async_copy(buf.at[:, :, pl.ds(start, width)], outs[i], sem.at[0, i]))
        copies.append(pltpu.make_async_copy(scale_ref.at[:, pl.ds(start, width)], scales[i], sem.at[1, i]))
        start += width
    for copy in copies:
        copy.start()
    for copy in copies:
        copy.wait()


def routed(n, one_query, other_query, one_key, other_key, one_value, other_value, mix_share, norm_gain):
    widths = (one_query.shape[1], one_key.shape[1], one_value.shape[1])
    rows, total = one_query.shape[0], sum(widths)
    pieces = len(plan(rows, n // 2, 0)[0])
    vmem = pl.BlockSpec(memory_space=pltpu.VMEM)
    hbm = pl.BlockSpec(memory_space=pl.ANY)
    buf, scale = pl.pallas_call(
        functools.partial(gather_kernel, n, widths),
        out_shape=(pltpu.VMEM((n, rows, total), jnp.bfloat16), pltpu.VMEM((1, total), jnp.float32)),
        in_specs=[hbm] * 8,
        out_specs=(vmem, vmem),
        scratch_shapes=[
            pltpu.VMEM((1, rows), jnp.float32),
            pltpu.VMEM((1, rows), jnp.float32),
            pltpu.VMEM((rows, total), jnp.float32),
            pltpu.VMEM((rows, total), jnp.float32),
            pltpu.VMEM((rows, LANES), jnp.float32),
            pltpu.VMEM((rows, LANES), jnp.float32),
            pltpu.VMEM((n, 1, total), jnp.float32),
            pltpu.VMEM((n // 2, 1, total), jnp.float32),
            pltpu.VMEM((3, MOST, total), jnp.float32),
            pltpu.SemaphoreType.DMA((2,)),
            pltpu.SemaphoreType.DMA((PARTS + 1, 2)),
            pltpu.SemaphoreType.DMA((3,)),
            pltpu.SemaphoreType.DMA((3,)),
            pltpu.SemaphoreType.DMA((3,)),
            pltpu.SemaphoreType.DMA((3, 2)),
            pltpu.SemaphoreType.DMA((n, pieces)),
            pltpu.SemaphoreType.REGULAR((2,)),
        ],
        compiler_params=pltpu.CompilerParams(collective_id=0, has_side_effects=True, vmem_limit_bytes=44 * 2**20),
    )(mix_share[None, :], norm_gain[None, :], one_query, other_query, one_key, other_key, one_value, other_value)
    outs = pl.pallas_call(
        functools.partial(store_kernel, widths),
        out_shape=tuple(jax.ShapeDtypeStruct((n, rows, width), jnp.bfloat16) for width in widths)
        + tuple(jax.ShapeDtypeStruct((1, width), jnp.float32) for width in widths),
        in_specs=[vmem, vmem],
        out_specs=(hbm,) * 6,
        scratch_shapes=[pltpu.SemaphoreType.DMA((2, 3))],
        compiler_params=pltpu.CompilerParams(vmem_limit_bytes=2**20),
    )(pltpu.with_memory_space_constraint(buf, pltpu.VMEM), pltpu.with_memory_space_constraint(scale, pltpu.VMEM))
    return tuple(out.reshape(n * rows, -1) for out in outs[:3]) + tuple(out[0] for out in outs[3:])


def solution(mesh):
    n = mesh.shape["shard"]

    def body(*args):
        return routed(n, *args) if fits(n, args[0].shape[0]) else plain(*args)

    return jax.shard_map(
        body,
        mesh=mesh,
        in_specs=(
            P("shard", "width"),
            P("shard", "width"),
            P("shard", "width"),
            P("shard", "width"),
            P("shard", "width"),
            P("shard", "width"),
            P("shard"),
            P("shard"),
        ),
        out_specs=(
            P(None, "width"),
            P(None, "width"),
            P(None, "width"),
            P("width"),
            P("width"),
            P("width"),
        ),
        check_vma=False,
    )
```

```python
import functools
import heapq

import jax
import jax.numpy as jnp
from jax import lax
from jax.experimental import pallas as pl
from jax.experimental.pallas import tpu as pltpu
from jax.sharding import PartitionSpec as P

MESH = pl.DeviceIdType.MESH
ROWS = 16
TILE = 8
LANES = 128
FIRST = ((16, 16, 16, 0), (16, 16, 16, 0))
LEADS = ((32, 32, 32, 16), (32, 32, 16, 16))
UP, DOWN, ACROSS = range(3)
PARTS = 5
MOST = max(map(max, LEADS))
START = 0
GAPS = ((0, 0), (2, 1))


def plain(one_query, other_query, one_key, other_key, one_value, other_value, mix_share, norm_gain):
    result_query = mix_share[:, None] * one_query + (1.0 - mix_share[:, None]) * other_query
    result_key = mix_share[:, None] * one_key + (1.0 - mix_share[:, None]) * other_key
    result_value = mix_share[:, None] * one_value + (1.0 - mix_share[:, None]) * other_value
    result_gained_query = result_query * norm_gain[:, None]
    result_gained_key = result_key * norm_gain[:, None]
    result_gained_value = result_value * norm_gain[:, None]
    total_query, total_key, total_value = lax.psum(
        (
            jnp.sum(result_gained_query * result_gained_query, axis=0),
            jnp.sum(result_gained_key * result_gained_key, axis=0),
            jnp.sum(result_gained_value * result_gained_value, axis=0),
        ),
        "shard",
    )
    scale_query = jnp.sqrt(total_query)
    scale_key = jnp.sqrt(total_key)
    scale_value = jnp.sqrt(total_value)
    narrow_query, narrow_key, narrow_value = (
        (result_gained_query / scale_query).astype(jnp.bfloat16),
        (result_gained_key / scale_key).astype(jnp.bfloat16),
        (result_gained_value / scale_value).astype(jnp.bfloat16),
    )
    final_query, final_key, final_value = (
        lax.all_gather(narrow_query, "shard", axis=0, tiled=True),
        lax.all_gather(narrow_key, "shard", axis=0, tiled=True),
        lax.all_gather(narrow_value, "shard", axis=0, tiled=True),
    )
    return (final_query, final_key, final_value, scale_query, scale_key, scale_value)


def cuts(start, end, parts, unit):
    edges = [start + (end - start) // unit * part // parts * unit for part in range(parts)] + [end]
    return [(low, high - low) for low, high in zip(edges, edges[1:])]


def table(values, z, line):
    return values[z] if z < 2 else values[max(z - line, -2)]


def plan(rows, line, core):
    half = rows // 2 // ROWS * ROWS
    leads = [table(LEADS[core], z, line) for z in range(line)]
    return [[(0, lead)] + cuts(lead, half, 2, ROWS) + [(half, rows - half)] for lead in leads]


def ways_from(z, line):
    return [way for way, ok in ((UP, z < line - 1), (DOWN, z > 0), (ACROSS, True)) if ok]


def early_from(z, line):
    return [way for way, ok in ((UP, z == line - 2), (DOWN, z == 1), (ACROSS, z in (0, line - 1))) if ok]


def relays(line, pieces):
    latency = 3 * TILE
    events, free, serial, order = [], {}, [], [[] for _ in range(line)]

    def send(time, z, way, column, source, c, early=False):
        target = (z + 1, z - 1, z)[way]
        if not early:
            time = free[z, way] = max(time, free.get((z, way), 0)) + pieces[source][c][1]
        serial.append(None)
        heapq.heappush(events, (time + latency * (not early), len(serial), target, column ^ (way == ACROSS), source, c, early))

    def onward(z, column, source, c):
        along = [UP] if (source < z or source == z == 0) and z < line - 1 else []
        along += [DOWN] if (source > z or source == z == line - 1) and z > 0 else []
        crosses = source not in (0, line - 1) or c < len(pieces[source]) - 1
        if column == 0:
            return along + ([ACROSS] if crosses else [])
        return [] if crosses else along

    for z in range(line):
        for way in ways_from(z, line):
            for c in range(len(pieces[z])):
                send(0, z, way, 0, z, c, c == 0 and way in early_from(z, line))
    while events:
        time, _, z, column, source, c, early = heapq.heappop(events)
        ways = onward(z, column, source, c)
        order[z].append((column, source, c, ways, early))
        for way in ways:
            send(time, z, way, column, source, c)
    return order


def sending(level, line, pieces, order):
    early, leaving = early_from(level, line), ways_from(level, line)
    sent = [[sum(size for _, size in pieces[level][way in early:]) if way in leaving else 0, 0] for way in range(3)]
    for _, source, c, ways, _ in order[level]:
        for way in ways:
            sent[way][1] += pieces[source][c][1]
    return sent


def folded(amount, rows, n):
    return next((d for d in range(1, n + 1) if amount % (d * TILE) == 0 and amount // d <= rows), None)


def fits(n, rows):
    if n % 2 or n < 8 or rows % ROWS or rows < 4 * MOST:
        return False
    line = n // 2
    plans = [plan(rows, line, core) for core in range(2)]
    orders = [relays(line, pieces) for pieces in plans]
    return all(folded(amount, rows, n) for pieces, order in zip(plans, orders)
        for z in range(line) for pair in sending(z, line, pieces, order) for amount in pair if amount)


def stages(rows):
    return [(0, MOST)] + cuts(MOST, rows, PARTS, ROWS)


def gather_kernel(n, widths, *refs):
    (share_hbm, gain_hbm), ins, (buf, scale_ref, share_ref, gain_ref, first, second, left, right, sums, pairs, early, row_sem, in_sem, sum_sem, early_send, early_recv, send_sem, recv_sem, token) = refs[:2], refs[2:8], refs[8:]
    rows = first.shape[0]
    total = sum(widths)
    line = n // 2
    me = lax.axis_index("shard")
    z, y = me // 2, me % 2
    other = z * 2 + 1 - y
    core = lax.axis_index("width") % 2
    plans = [plan(rows, line, k) for k in range(2)]
    orders = [relays(line, pieces) for pieces in plans]
    up, down, always = z < line - 1, z > 0, z >= 0
    conditions = (up, down, always)
    targets = (jnp.minimum(z + 1, line - 1) * 2 + y, jnp.maximum(z - 1, 0) * 2 + y, other)
    starts = [sum(widths[:i]) for i in range(len(widths))]

    vectors = [
        pltpu.make_async_copy(source, dest, row_sem.at[i])
        for i, (source, dest) in enumerate(((share_hbm, share_ref), (gain_hbm, gain_ref)))
    ]
    for copy in vectors:
        copy.start()
    parts = stages(rows)

    def load(p):
        low, size = parts[p]
        for i, ref in enumerate(ins):
            dest = (first, second)[i % 2].at[pl.ds(low, size), pl.ds(starts[i // 2], widths[i // 2])]
            pltpu.make_async_copy(ref.at[pl.ds(low, size), :], dest, in_sem.at[p, i % 2]).start()

    def loaded(p):
        for i, ref in enumerate((first, second)):
            whole = ref.at[pl.ds(parts[p][0], parts[p][1]), :]
            pltpu.make_async_copy(whole, whole, in_sem.at[p, i]).wait()

    load(0)

    barrier = pltpu.get_barrier_semaphore()
    for way, condition in enumerate(conditions):
        @pl.when(condition)
        def _():
            pl.semaphore_signal(barrier, inc=1, device_id={"shard": targets[way]}, device_id_type=MESH)

    for p in range(1, len(parts)):
        load(p)

    for copy in vectors:
        copy.wait()
    for low in range(0, rows, LANES):
        size = min(LANES, rows - low)
        share, gain = share_ref[:, low:low + size], gain_ref[:, low:low + size]
        for ref, row in ((left, share * gain), (right, (1.0 - share) * gain)):
            ref[pl.ds(low, size), :] = jnp.transpose(jnp.broadcast_to(row, (LANES, size)))

    def mixed(block, acc):
        at = pl.ds(pl.multiple_of(block * ROWS, ROWS), ROWS)
        ours, theirs = (jnp.concatenate([ref[at, :]] * 4, axis=1) for ref in (left, right))
        out = []
        for i in range(len(acc)):
            cols = pl.ds(i * 512, 512)
            value = ours * first[at, cols] + theirs * second[at, cols]
            first[at, cols] = value
            square = value * value
            out.append(acc[i] + square[:8] + square[8:])
        return tuple(out)

    def early_copy(way, low, size):
        return pltpu.make_async_remote_copy(
            src_ref=first.at[pl.ds(low, size), :], dst_ref=early.at[way, pl.ds(low, size), :],
            send_sem=early_send.at[way], recv_sem=early_recv.at[way],
            device_id={"shard": targets[way]}, device_id_type=MESH)

    def start_early(level, ways, low, end):
        for way in ways:
            if way in early_from(level, line) and end > low:
                early_copy(way, low, end - low).start()

    def each_level(act):
        for k in range(2):
            for level in range(line):
                @pl.when((z == level) & (core == k))
                def _():
                    act(level, k)

    def wait_token(level, way):
        if ways_from(level, line).count(1 - way):
            pl.semaphore_wait(token.at[way], 1)

    def send_token(level, way):
        if way in ways_from(level, line):
            pl.semaphore_signal(token.at[way], inc=1, device_id={"shard": targets[way]}, device_id_type=MESH)

    def begun(level, k):
        pl.semaphore_wait(barrier, len(ways_from(level, line)))
        start_early(level, (UP, DOWN, ACROSS), 0, table(FIRST[k], level, line))
        if level == line - 1:
            send_token(level, DOWN)

    def risen(level):
        wait_token(level, UP)
        send_token(level, UP)

    acc = tuple(jnp.zeros((8, 512), jnp.float32) for _ in range(total // 512))
    for p, (low, size) in enumerate(parts):
        loaded(p)
        acc = lax.fori_loop(low // ROWS, (low + size) // ROWS, mixed, acc)
        if p == START:
            each_level(begun)
        for level in range(line):
            if p == min(max(2 * level - 1, 0), len(parts) - 1):
                @pl.when(z == level)
                def _():
                    risen(level)
    for i, value in enumerate(acc):
        sums[me, :, pl.ds(i * 512, 512)] = jnp.sum(value, axis=0, keepdims=True)

    def sum_copy(target, ref, k):
        return pltpu.make_async_remote_copy(
            src_ref=ref, dst_ref=ref, send_sem=sum_sem.at[0], recv_sem=sum_sem.at[k],
            device_id={"shard": target}, device_id_type=MESH)

    def exchanged(level, k):
        first_early, last_early = table(FIRST[k], level, line), plans[k][level][0][1]

        def paired():
            sum_copy(other, sums.at[other], 1).wait_recv()
            pairs[level] = sums[level * 2] + sums[level * 2 + 1]

        def lift(above):
            sum_copy(above * 2 + y, pairs.at[level], 2).start()

        for below in range(level):
            for side in (1 - y, y):
                sum_copy(below * 2 + side, sums.at[me], 2).start()
        sum_copy(other, sums.at[me], 1).start()
        start_early(level, (DOWN, ACROSS), first_early, last_early)
        if level == 0:
            paired()
            lift(1)
        wait_token(level, DOWN)
        if level < line - 1:
            send_token(level, DOWN)
        if level > 0:
            paired()
        for above in range(line - 1, max(level, 1) if level == 0 else level, -1):
            lift(above)
        start_early(level, (UP,), first_early, last_early)
        sum_copy(other, sums.at[pl.ds(0, 2 * (line - 1 - level) + level)], 2).wait_recv()
        for above in range(level + 1, line):
            pairs[above] = sums[above * 2] + sums[above * 2 + 1]
        sum_copy(other, sums.at[pl.ds(0, 2 * level + line - level)], 2).wait_send()

    each_level(exchanged)
    whole = pairs[0]
    for level in range(1, line):
        whole = whole + pairs[level]
    scale = jnp.sqrt(whole)
    scale_ref[...] = scale
    inverse = jnp.broadcast_to(1.0 / scale, (8, total))

    def scaled(source, ref):
        def step(block, carry):
            at = pl.ds(pl.multiple_of(block * ROWS, ROWS), ROWS)
            for i in range(total // 512):
                cols = pl.ds(i * 512, 512)
                wide = jnp.concatenate([inverse[:, i * 512:(i + 1) * 512]] * 2, axis=0)
                buf[source, at, cols] = (ref[at, cols] * wide).astype(buf.dtype)
            return carry
        return step

    def copy(way, source, piece, c, own=False):
        low, size = piece
        ref = buf.at[source, pl.ds(low, size), :]
        return pltpu.make_async_remote_copy(
            src_ref=ref, dst_ref=ref, send_sem=send_sem.at[way, 0 if own else 1], recv_sem=recv_sem.at[source, c],
            device_id={"shard": targets[way]}, device_id_type=MESH)

    def rest(level, k):
        pieces, order = plans[k], orders[k]
        leaving, early_ways = ways_from(level, line), early_from(level, line)

        def scale_rows(source, ref, low, size):
            lax.fori_loop(low // ROWS, (low + size) // ROWS, scaled(source, ref), 0)

        gaps = GAPS[k][level] if level < 2 else 0
        last = len(pieces[level]) - 1
        events = [(1, level, last - 1), (1, level, last)][:gaps]
        held = []

        def issue_own(c):
            for way in leaving:
                if c == last and way in early_ways and gaps:
                    held.append((way, me, pieces[level][c], c, True))
                elif c or way not in early_ways:
                    copy(way, me, pieces[level][c], c, True).start()

        for c in (1, 0, 2, 3):
            scale_rows(me, first, *pieces[level][c])
            if c != 1:
                issue_own(1 if c == 0 else 0 if c == 2 else 2)
        issue_own(last)

        came = ((level + 1, DOWN, me + 2), (level - 1, UP, me - 2), (level, ACROSS, other))
        for at, slot, source in came:
            if 0 <= at < line and slot in early_from(at, line):
                piece = pieces[at][0]
                early_copy(slot, *piece).wait_recv()
                scale_rows(source, early.at[slot], *piece)

        for column, at, c, ways, direct in order[level]:
            source = at * 2 + (1 - y if column else y)
            if not direct:
                copy(ACROSS, source, pieces[at][c], c).wait_recv()
            for way in ways:
                if events and way in early_ways:
                    held.append((way, source, pieces[at][c], c))
                else:
                    copy(way, source, pieces[at][c], c).start()
            if events and (column, at, c) == events[0]:
                events.pop(0)
                ready = 1 if events else len(held)
                for args in held[:ready]:
                    copy(*args).start()
                del held[:ready]
        amounts = sending(level, line, pieces, order)
        for way, relayed in ((way, relayed) for way in leaving for relayed in range(2)):
            amount = amounts[way][relayed]
            if amount:
                depth = folded(amount, rows, n)
                ref = buf.at[pl.ds(0, depth), pl.ds(0, amount // depth), :]
                pltpu.make_async_remote_copy(
                    src_ref=ref, dst_ref=ref, send_sem=send_sem.at[way, relayed], recv_sem=recv_sem.at[0, 0],
                    device_id={"shard": targets[way]}, device_id_type=MESH).wait_send()
        for way in early_ways:
            early_copy(way, *pieces[level][0]).wait_send()

    each_level(rest)


def store_kernel(widths, buf, scale_ref, *refs):
    outs, scales, sem = refs[:3], refs[3:6], refs[6]
    start = 0
    waits = []
    for i, width in enumerate(widths):
        cols = pl.ds(start, width)
        for source in range(buf.shape[0]):
            pltpu.make_async_copy(buf.at[source, :, cols], outs[i].at[source], sem.at[0, i]).start()
        pltpu.make_async_copy(scale_ref.at[:, cols], scales[i], sem.at[1, i]).start()
        waits.append(pltpu.make_async_copy(buf.at[:, :, cols], outs[i], sem.at[0, i]))
        waits.append(pltpu.make_async_copy(scale_ref.at[:, cols], scales[i], sem.at[1, i]))
        start += width
    for copy in waits:
        copy.wait()


def routed(n, one_query, other_query, one_key, other_key, one_value, other_value, mix_share, norm_gain):
    widths = (one_query.shape[1], one_key.shape[1], one_value.shape[1])
    rows, total = one_query.shape[0], sum(widths)
    pieces = len(plan(rows, n // 2, 0)[0])
    vmem = pl.BlockSpec(memory_space=pltpu.VMEM)
    hbm = pl.BlockSpec(memory_space=pl.ANY)
    buf, scale = pl.pallas_call(
        functools.partial(gather_kernel, n, widths),
        out_shape=(pltpu.VMEM((n, rows, total), jnp.bfloat16), pltpu.VMEM((1, total), jnp.float32)),
        in_specs=[hbm] * 8,
        out_specs=(vmem, vmem),
        scratch_shapes=[
            pltpu.VMEM((1, rows), jnp.float32),
            pltpu.VMEM((1, rows), jnp.float32),
            pltpu.VMEM((rows, total), jnp.float32),
            pltpu.VMEM((rows, total), jnp.float32),
            pltpu.VMEM((rows, LANES), jnp.float32),
            pltpu.VMEM((rows, LANES), jnp.float32),
            pltpu.VMEM((n, 1, total), jnp.float32),
            pltpu.VMEM((n // 2, 1, total), jnp.float32),
            pltpu.VMEM((3, MOST, total), jnp.float32),
            pltpu.SemaphoreType.DMA((2,)),
            pltpu.SemaphoreType.DMA((PARTS + 1, 2)),
            pltpu.SemaphoreType.DMA((3,)),
            pltpu.SemaphoreType.DMA((3,)),
            pltpu.SemaphoreType.DMA((3,)),
            pltpu.SemaphoreType.DMA((3, 2)),
            pltpu.SemaphoreType.DMA((n, pieces)),
            pltpu.SemaphoreType.REGULAR((2,)),
        ],
        compiler_params=pltpu.CompilerParams(collective_id=0, has_side_effects=True, vmem_limit_bytes=44 * 2**20),
    )(mix_share[None, :], norm_gain[None, :], one_query, other_query, one_key, other_key, one_value, other_value)
    outs = pl.pallas_call(
        functools.partial(store_kernel, widths),
        out_shape=tuple(jax.ShapeDtypeStruct((n, rows, width), jnp.bfloat16) for width in widths)
        + tuple(jax.ShapeDtypeStruct((1, width), jnp.float32) for width in widths),
        in_specs=[vmem, vmem],
        out_specs=(hbm,) * 6,
        scratch_shapes=[pltpu.SemaphoreType.DMA((2, 3))],
        compiler_params=pltpu.CompilerParams(vmem_limit_bytes=2**20),
    )(pltpu.with_memory_space_constraint(buf, pltpu.VMEM), pltpu.with_memory_space_constraint(scale, pltpu.VMEM))
    return tuple(out.reshape(n * rows, -1) for out in outs[:3]) + tuple(out[0] for out in outs[3:])


def solution(mesh):
    n = mesh.shape["shard"]

    def body(*args):
        return routed(n, *args) if fits(n, args[0].shape[0]) else plain(*args)

    return jax.shard_map(
        body,
        mesh=mesh,
        in_specs=(
            P("shard", "width"),
            P("shard", "width"),
            P("shard", "width"),
            P("shard", "width"),
            P("shard", "width"),
            P("shard", "width"),
            P("shard"),
            P("shard"),
        ),
        out_specs=(
            P(None, "width"),
            P(None, "width"),
            P(None, "width"),
            P("width"),
            P("width"),
            P("width"),
        ),
        check_vma=False,
    )
```

```python
import functools
import heapq

import jax
import jax.numpy as jnp
from jax import lax
from jax.experimental import pallas as pl
from jax.experimental.pallas import tpu as pltpu
from jax.sharding import PartitionSpec as P

MESH = pl.DeviceIdType.MESH
ROWS = 16
TILE = 8
LANES = 128
FIRST = ((16, 16, 16, 0), (16, 16, 16, 0))
LEADS = ((32, 32, 32, 16), (32, 32, 16, 16))
UP, DOWN, ACROSS = range(3)
PARTS = 5
MOST = max(map(max, LEADS))
START = 0
GAPS = ((0, 0), (2, 1))


def plain(one_query, other_query, one_key, other_key, one_value, other_value, mix_share, norm_gain):
    result_query = mix_share[:, None] * one_query + (1.0 - mix_share[:, None]) * other_query
    result_key = mix_share[:, None] * one_key + (1.0 - mix_share[:, None]) * other_key
    result_value = mix_share[:, None] * one_value + (1.0 - mix_share[:, None]) * other_value
    result_gained_query = result_query * norm_gain[:, None]
    result_gained_key = result_key * norm_gain[:, None]
    result_gained_value = result_value * norm_gain[:, None]
    total_query, total_key, total_value = lax.psum(
        (
            jnp.sum(result_gained_query * result_gained_query, axis=0),
            jnp.sum(result_gained_key * result_gained_key, axis=0),
            jnp.sum(result_gained_value * result_gained_value, axis=0),
        ),
        "shard",
    )
    scale_query = jnp.sqrt(total_query)
    scale_key = jnp.sqrt(total_key)
    scale_value = jnp.sqrt(total_value)
    narrow_query, narrow_key, narrow_value = (
        (result_gained_query / scale_query).astype(jnp.bfloat16),
        (result_gained_key / scale_key).astype(jnp.bfloat16),
        (result_gained_value / scale_value).astype(jnp.bfloat16),
    )
    final_query, final_key, final_value = (
        lax.all_gather(narrow_query, "shard", axis=0, tiled=True),
        lax.all_gather(narrow_key, "shard", axis=0, tiled=True),
        lax.all_gather(narrow_value, "shard", axis=0, tiled=True),
    )
    return (final_query, final_key, final_value, scale_query, scale_key, scale_value)


def cuts(start, end, parts, unit):
    edges = [start + (end - start) // unit * part // parts * unit for part in range(parts)] + [end]
    return [(low, high - low) for low, high in zip(edges, edges[1:])]


def table(values, z, line):
    return values[z] if z < 2 else values[max(z - line, -2)]


def plan(rows, line, core):
    half = rows // 2 // ROWS * ROWS
    leads = [table(LEADS[core], z, line) for z in range(line)]
    return [[(0, lead), (lead, 3 * ROWS), (lead + 3 * ROWS, half - lead - 3 * ROWS), (half, rows - half)] for lead in leads]


def ways_from(z, line):
    return [way for way, ok in ((UP, z < line - 1), (DOWN, z > 0), (ACROSS, True)) if ok]


def early_from(z, line):
    return [way for way, ok in ((UP, z == line - 2), (DOWN, z == 1), (ACROSS, z in (0, line - 1))) if ok]


def relays(line, pieces):
    latency = 3 * TILE
    events, free, serial, order = [], {}, [], [[] for _ in range(line)]

    def send(time, z, way, column, source, c, early=False):
        target = (z + 1, z - 1, z)[way]
        if not early:
            time = free[z, way] = max(time, free.get((z, way), 0)) + pieces[source][c][1]
        serial.append(None)
        heapq.heappush(events, (time + latency * (not early), len(serial), target, column ^ (way == ACROSS), source, c, early))

    def onward(z, column, source, c):
        along = [UP] if (source < z or source == z == 0) and z < line - 1 else []
        along += [DOWN] if (source > z or source == z == line - 1) and z > 0 else []
        crosses = source not in (0, line - 1) or c < len(pieces[source]) - 1
        if column == 0:
            return along + ([ACROSS] if crosses else [])
        return [] if crosses else along

    for z in range(line):
        for way in ways_from(z, line):
            for c in range(len(pieces[z])):
                send(0, z, way, 0, z, c, c == 0 and way in early_from(z, line))
    while events:
        time, _, z, column, source, c, early = heapq.heappop(events)
        ways = onward(z, column, source, c)
        order[z].append((column, source, c, ways, early))
        for way in ways:
            send(time, z, way, column, source, c)
    return order


def sending(level, line, pieces, order):
    early, leaving = early_from(level, line), ways_from(level, line)
    sent = [[sum(size for _, size in pieces[level][way in early:]) if way in leaving else 0, 0] for way in range(3)]
    for _, source, c, ways, _ in order[level]:
        for way in ways:
            sent[way][1] += pieces[source][c][1]
    return sent


def folded(amount, rows, n):
    return next((d for d in range(1, n + 1) if amount % (d * TILE) == 0 and amount // d <= rows), None)


def fits(n, rows):
    if n % 2 or n < 8 or rows % ROWS or rows < 4 * MOST:
        return False
    line = n // 2
    plans = [plan(rows, line, core) for core in range(2)]
    orders = [relays(line, pieces) for pieces in plans]
    return all(folded(amount, rows, n) for pieces, order in zip(plans, orders)
        for z in range(line) for pair in sending(z, line, pieces, order) for amount in pair if amount)


def stages(rows):
    return [(0, MOST)] + cuts(MOST, rows, PARTS, ROWS)


def gather_kernel(n, widths, *refs):
    (share_hbm, gain_hbm), ins, (buf, scale_ref, share_ref, gain_ref, both, left, right, sums, pairs, early, row_sem, in_sem, sum_sem, early_send, early_recv, send_sem, recv_sem, token) = refs[:2], refs[2:8], refs[8:]
    first, second = both.at[0], both.at[1]
    rows = both.shape[1]
    total = sum(widths)
    line = n // 2
    me = lax.axis_index("shard")
    z, y = me // 2, me % 2
    other = z * 2 + 1 - y
    core = lax.axis_index("width") % 2
    plans = [plan(rows, line, k) for k in range(2)]
    orders = [relays(line, pieces) for pieces in plans]
    up, down, always = z < line - 1, z > 0, z >= 0
    conditions = (up, down, always)
    targets = (jnp.minimum(z + 1, line - 1) * 2 + y, jnp.maximum(z - 1, 0) * 2 + y, other)
    starts = [sum(widths[:i]) for i in range(len(widths))]

    vectors = [
        pltpu.make_async_copy(source, dest, row_sem.at[i])
        for i, (source, dest) in enumerate(((share_hbm, share_ref), (gain_hbm, gain_ref)))
    ]
    for copy in vectors:
        copy.start()
    parts = stages(rows)

    def load(p):
        low, size = parts[p]
        for i, ref in enumerate(ins):
            dest = (first, second)[i % 2].at[pl.ds(low, size), pl.ds(starts[i // 2], widths[i // 2])]
            pltpu.make_async_copy(ref.at[pl.ds(low, size), :], dest, in_sem.at[p]).start()

    def loaded(p):
        whole = both.at[:, pl.ds(parts[p][0], parts[p][1]), :]
        pltpu.make_async_copy(whole, whole, in_sem.at[p]).wait()

    load(0)

    barrier = pltpu.get_barrier_semaphore()
    for way, condition in enumerate(conditions):
        @pl.when(condition)
        def _():
            pl.semaphore_signal(barrier, inc=1, device_id={"shard": targets[way]}, device_id_type=MESH)

    for p in range(1, len(parts)):
        load(p)

    for copy in vectors:
        copy.wait()
    for low in range(0, rows, LANES):
        size = min(LANES, rows - low)
        share, gain = share_ref[:, low:low + size], gain_ref[:, low:low + size]
        for ref, row in ((left, share * gain), (right, (1.0 - share) * gain)):
            ref[pl.ds(low, size), :] = jnp.transpose(jnp.broadcast_to(row, (LANES, size)))

    def mixed(block, acc):
        at = pl.ds(pl.multiple_of(block * ROWS, ROWS), ROWS)
        ours, theirs = (jnp.concatenate([ref[at, :]] * 4, axis=1) for ref in (left, right))
        out = []
        for i in range(len(acc)):
            cols = pl.ds(i * 512, 512)
            value = ours * first[at, cols] + theirs * second[at, cols]
            first[at, cols] = value
            square = value * value
            out.append(acc[i] + square[:8] + square[8:])
        return tuple(out)

    def early_copy(way, low, size):
        return pltpu.make_async_remote_copy(
            src_ref=first.at[pl.ds(low, size), :], dst_ref=early.at[way, pl.ds(low, size), :],
            send_sem=early_send.at[way], recv_sem=early_recv.at[way],
            device_id={"shard": targets[way]}, device_id_type=MESH)

    def start_early(level, ways, low, end):
        for way in ways:
            if way in early_from(level, line) and end > low:
                early_copy(way, low, end - low).start()

    def each_level(act):
        for k in range(2):
            for level in range(line):
                @pl.when((z == level) & (core == k))
                def _():
                    act(level, k)

    def wait_token(level, way):
        if ways_from(level, line).count(1 - way):
            pl.semaphore_wait(token.at[way], 1)

    def send_token(level, way):
        if way in ways_from(level, line):
            pl.semaphore_signal(token.at[way], inc=1, device_id={"shard": targets[way]}, device_id_type=MESH)

    def begun(level, k):
        pl.semaphore_wait(barrier, len(ways_from(level, line)))
        start_early(level, (UP, DOWN, ACROSS), 0, table(FIRST[k], level, line))
        if level == line - 1:
            send_token(level, DOWN)

    def risen(level):
        wait_token(level, UP)
        send_token(level, UP)

    acc = tuple(jnp.zeros((8, 512), jnp.float32) for _ in range(total // 512))
    for p, (low, size) in enumerate(parts):
        loaded(p)
        acc = lax.fori_loop(low // ROWS, (low + size) // ROWS, mixed, acc)
        if p == START:
            each_level(begun)
        for level in range(line):
            if p == min(max(2 * level - 1, 0), len(parts) - 1):
                @pl.when(z == level)
                def _():
                    risen(level)
    for i, value in enumerate(acc):
        sums[me, :, pl.ds(i * 512, 512)] = jnp.sum(value, axis=0, keepdims=True)

    def sum_copy(target, ref, k):
        return pltpu.make_async_remote_copy(
            src_ref=ref, dst_ref=ref, send_sem=sum_sem.at[0], recv_sem=sum_sem.at[k],
            device_id={"shard": target}, device_id_type=MESH)

    def exchanged(level, k):
        first_early, last_early = table(FIRST[k], level, line), plans[k][level][0][1]

        def paired():
            sum_copy(other, sums.at[other], 1).wait_recv()
            pairs[level] = sums[level * 2] + sums[level * 2 + 1]

        def lift(above):
            sum_copy(above * 2 + y, pairs.at[level], 2).start()

        for below in range(level):
            for side in (1 - y, y):
                sum_copy(below * 2 + side, sums.at[me], 2).start()
        sum_copy(other, sums.at[me], 1).start()
        start_early(level, (DOWN, ACROSS), first_early, last_early)
        if level == 0:
            paired()
            lift(1)
        wait_token(level, DOWN)
        if level < line - 1:
            send_token(level, DOWN)
        if level > 0:
            paired()
        for above in range(line - 1, max(level, 1) if level == 0 else level, -1):
            lift(above)
        start_early(level, (UP,), first_early, last_early)
        sum_copy(other, sums.at[pl.ds(0, 2 * (line - 1 - level) + level)], 2).wait_recv()
        for above in range(level + 1, line):
            pairs[above] = sums[above * 2] + sums[above * 2 + 1]
        sum_copy(other, sums.at[pl.ds(0, 2 * level + line - level)], 2).wait_send()

    each_level(exchanged)
    whole = pairs[0]
    for level in range(1, line):
        whole = whole + pairs[level]
    scale = jnp.sqrt(whole)
    scale_ref[...] = scale
    inverse = jnp.broadcast_to(1.0 / scale, (8, total))

    def scaled(source, ref):
        def step(block, carry):
            at = pl.ds(pl.multiple_of(block * ROWS, ROWS), ROWS)
            for i in range(total // 512):
                cols = pl.ds(i * 512, 512)
                wide = jnp.concatenate([inverse[:, i * 512:(i + 1) * 512]] * 2, axis=0)
                buf[source, at, cols] = (ref[at, cols] * wide).astype(buf.dtype)
            return carry
        return step

    def copy(way, source, piece, c, own=False):
        low, size = piece
        ref = buf.at[source, pl.ds(low, size), :]
        return pltpu.make_async_remote_copy(
            src_ref=ref, dst_ref=ref, send_sem=send_sem.at[way, 0 if own else 1], recv_sem=recv_sem.at[source, c],
            device_id={"shard": targets[way]}, device_id_type=MESH)

    def rest(level, k):
        pieces, order = plans[k], orders[k]
        leaving, early_ways = ways_from(level, line), early_from(level, line)

        def scale_rows(source, ref, low, size):
            lax.fori_loop(low // ROWS, (low + size) // ROWS, scaled(source, ref), 0)

        gaps = GAPS[k][level] if level < 2 else 0
        last = len(pieces[level]) - 1
        events = [(1, level, last - 1), (1, level, last)][:gaps]
        held = []

        def issue_own(c):
            for way in leaving:
                if c == last and way in early_ways and gaps:
                    held.append((way, me, pieces[level][c], c, True))
                elif c or way not in early_ways:
                    copy(way, me, pieces[level][c], c, True).start()

        for c in (1, 0, 2, 3):
            scale_rows(me, first, *pieces[level][c])
            if c != 1:
                issue_own(1 if c == 0 else 0 if c == 2 else 2)
        issue_own(last)

        came = ((level + 1, DOWN, me + 2), (level - 1, UP, me - 2), (level, ACROSS, other))
        for at, slot, source in came:
            if 0 <= at < line and slot in early_from(at, line):
                piece = pieces[at][0]
                early_copy(slot, *piece).wait_recv()
                scale_rows(source, early.at[slot], *piece)

        for column, at, c, ways, direct in order[level]:
            source = at * 2 + (1 - y if column else y)
            if not direct:
                copy(ACROSS, source, pieces[at][c], c).wait_recv()
            for way in ways:
                if events and way in early_ways:
                    held.append((way, source, pieces[at][c], c))
                else:
                    copy(way, source, pieces[at][c], c).start()
            if events and (column, at, c) == events[0]:
                events.pop(0)
                ready = 1 if events else len(held)
                for args in held[:ready]:
                    copy(*args).start()
                del held[:ready]
        amounts = sending(level, line, pieces, order)
        for way, relayed in ((way, relayed) for way in leaving for relayed in range(2)):
            amount = amounts[way][relayed]
            if amount:
                depth = folded(amount, rows, n)
                ref = buf.at[pl.ds(0, depth), pl.ds(0, amount // depth), :]
                pltpu.make_async_remote_copy(
                    src_ref=ref, dst_ref=ref, send_sem=send_sem.at[way, relayed], recv_sem=recv_sem.at[0, 0],
                    device_id={"shard": targets[way]}, device_id_type=MESH).wait_send()
        for way in early_ways:
            early_copy(way, *pieces[level][0]).wait_send()

    each_level(rest)


def store_kernel(widths, buf, scale_ref, *refs):
    outs, scales, sem = refs[:3], refs[3:6], refs[6]
    start = 0
    waits = []
    for i, width in enumerate(widths):
        cols = pl.ds(start, width)
        for source in range(buf.shape[0]):
            pltpu.make_async_copy(buf.at[source, :, cols], outs[i].at[source], sem.at[0, i]).start()
        pltpu.make_async_copy(scale_ref.at[:, cols], scales[i], sem.at[1, i]).start()
        waits.append(pltpu.make_async_copy(buf.at[:, :, cols], outs[i], sem.at[0, i]))
        waits.append(pltpu.make_async_copy(scale_ref.at[:, cols], scales[i], sem.at[1, i]))
        start += width
    for copy in waits:
        copy.wait()


def routed(n, one_query, other_query, one_key, other_key, one_value, other_value, mix_share, norm_gain):
    widths = (one_query.shape[1], one_key.shape[1], one_value.shape[1])
    rows, total = one_query.shape[0], sum(widths)
    pieces = len(plan(rows, n // 2, 0)[0])
    vmem = pl.BlockSpec(memory_space=pltpu.VMEM)
    hbm = pl.BlockSpec(memory_space=pl.ANY)
    buf, scale = pl.pallas_call(
        functools.partial(gather_kernel, n, widths),
        out_shape=(pltpu.VMEM((n, rows, total), jnp.bfloat16), pltpu.VMEM((1, total), jnp.float32)),
        in_specs=[hbm] * 8,
        out_specs=(vmem, vmem),
        scratch_shapes=[
            pltpu.VMEM((1, rows), jnp.float32),
            pltpu.VMEM((1, rows), jnp.float32),
            pltpu.VMEM((2, rows, total), jnp.float32),
            pltpu.VMEM((rows, LANES), jnp.float32),
            pltpu.VMEM((rows, LANES), jnp.float32),
            pltpu.VMEM((n, 1, total), jnp.float32),
            pltpu.VMEM((n // 2, 1, total), jnp.float32),
            pltpu.VMEM((3, MOST, total), jnp.float32),
            pltpu.SemaphoreType.DMA((2,)),
            pltpu.SemaphoreType.DMA((PARTS + 1,)),
            pltpu.SemaphoreType.DMA((3,)),
            pltpu.SemaphoreType.DMA((3,)),
            pltpu.SemaphoreType.DMA((3,)),
            pltpu.SemaphoreType.DMA((3, 2)),
            pltpu.SemaphoreType.DMA((n, pieces)),
            pltpu.SemaphoreType.REGULAR((2,)),
        ],
        compiler_params=pltpu.CompilerParams(collective_id=0, has_side_effects=True, vmem_limit_bytes=44 * 2**20),
    )(mix_share[None, :], norm_gain[None, :], one_query, other_query, one_key, other_key, one_value, other_value)
    outs = pl.pallas_call(
        functools.partial(store_kernel, widths),
        out_shape=tuple(jax.ShapeDtypeStruct((n, rows, width), jnp.bfloat16) for width in widths)
        + tuple(jax.ShapeDtypeStruct((1, width), jnp.float32) for width in widths),
        in_specs=[vmem, vmem],
        out_specs=(hbm,) * 6,
        scratch_shapes=[pltpu.SemaphoreType.DMA((2, 3))],
        compiler_params=pltpu.CompilerParams(vmem_limit_bytes=2**20),
    )(pltpu.with_memory_space_constraint(buf, pltpu.VMEM), pltpu.with_memory_space_constraint(scale, pltpu.VMEM))
    return tuple(out.reshape(n * rows, -1) for out in outs[:3]) + tuple(out[0] for out in outs[3:])


def solution(mesh):
    n = mesh.shape["shard"]

    def body(*args):
        return routed(n, *args) if fits(n, args[0].shape[0]) else plain(*args)

    return jax.shard_map(
        body,
        mesh=mesh,
        in_specs=(
            P("shard", "width"),
            P("shard", "width"),
            P("shard", "width"),
            P("shard", "width"),
            P("shard", "width"),
            P("shard", "width"),
            P("shard"),
            P("shard"),
        ),
        out_specs=(
            P(None, "width"),
            P(None, "width"),
            P(None, "width"),
            P("width"),
            P("width"),
            P("width"),
        ),
        check_vma=False,
    )
```
